256 devices in a mesh: pipe: 8 (over x, z_lo), tensor: 4 (over y), expert: 8 (over z_hi, core).
Axes of the slice: x: 4, y: 4, z: 8 (z_hi: 4, z_lo: 2; z = z_hi * 2 + z_lo), core: 2. Of those that a mesh axis runs over, the one named last changes fastest.
Arguments:
- tokens: bfloat16 [2, 512, 4096], P(None, 'expert'), may hold values from -6 to 6
- gains: float32 [8, 4096], P('pipe'), may hold values from 0.1 to 1.9
- route_ids: int32 [8, 2, 512, 2], P('pipe', None, 'expert'), may hold values from 0 to 7, all different within a row
- route_weights: float32 [8, 2, 512, 2], P('pipe', None, 'expert'), may hold values from 0.2 to 1
- picks: int32 [8, 2, 8, 64], P('pipe', None, 'expert'), may hold values from 0 to 63, each once within a row
- w_gate: bfloat16 [8, 8, 4096, 1536], P('pipe', 'expert', None, 'tensor'), may hold values from -0.09375 to 0.09375
- w_up: bfloat16 [8, 8, 4096, 1536], P('pipe', 'expert', None, 'tensor'), may hold values from -0.09375 to 0.09375
- w_down: bfloat16 [8, 8, 1536, 4096], P('pipe', 'expert', 'tensor'), may hold values from -0.15625 to 0.15625
Outputs:
- streams: bfloat16 [8, 2, 512, 4096], P('pipe', None, 'expert', 'tensor')
The draws below stay inside these ranges and needn't reach their ends.
Inputs may be any that keep to these rules, and one draw needn't show every extreme that they name: `route_ids`: each token names 2 different experts; every expert is named by some token. `picks`: for every layer, micro-batch and block of 64 tokens, a permutation of 0 to 63.
All inputs are finite; a program needn't handle non-finite values.
Results may differ from the reference program's by a relative error of at most 0.025.
Values may be sent and summed in bfloat16 or wider, within the bound.
A program may use at most 64 MiB of HBM per device.

```python
import jax
import jax.numpy as jnp
from jax import lax

D = 4096
FF = 1536
TOPK = 2
MICRO = 2
TOK_DEV = 64
EXPERTS = 8
QUARTER = 16
CAP = 5
TOKENS = 512
N_PIPE = 8
N_TENSOR = 4
N_EXPERT = 8


def steps_of(rng, shape, shards, low, top_value):
    loudness, own = 1.0, jax.random.fold_in(rng, 6)
    for dim, parts in shards:
        steps = jnp.exp(jax.random.uniform(jax.random.fold_in(own, dim), (parts,), jnp.float32, low / len(shards), top_value / len(shards)))
        loudness = loudness * jnp.repeat(steps, shape[dim] // parts).reshape([-1 if axis == dim else 1 for axis in range(len(shape))])
    return loudness


def different_ones(stream_key, rows, number_of, top, lift):
    sequence = jax.random.permutation(jax.random.fold_in(stream_key, 1), number_of)
    pull = sequence
    for power in range(3):
        pull = pull * pull // number_of
    pull = pull * lift // number_of
    lots = jax.random.randint(jax.random.fold_in(stream_key, 2), (rows, number_of), 0, 4096) + pull
    fixed_rows = jax.random.permutation(jax.random.fold_in(stream_key, 3), rows)[jnp.arange(number_of) % rows]
    lots = jnp.where(jnp.arange(rows)[:, None] == fixed_rows[None, :], 1 << 14, lots)
    priority = lots * number_of + jnp.arange(number_of)
    return lax.top_k(priority.astype(jnp.int32), top)[1].astype(jnp.int32)


def gaussian(key, shape, deviation, most, pieces=(), kind=jnp.bfloat16):
    values = jax.random.normal(key, shape, jnp.float32) * deviation
    if len(pieces) > 0:
        values = steps_of(key, shape, pieces, -0.22, 0.18) * values
    return jnp.clip(values, min=-most, max=most).astype(kind)


def setup_inputs(seed: int = 0) -> dict:
    key_list = jax.random.split(jax.random.key(seed), 9)
    tokens = gaussian(key_list[0], (MICRO, TOKENS, D), 1.0, 6.0, ((1, 8),))
    gains = jnp.clip(1.0 + 0.18 * jax.random.normal(key_list[1], (N_PIPE, D), jnp.float32), 0.1, 1.9)
    route_ids = different_ones(key_list[2], N_PIPE * MICRO * TOKENS, EXPERTS, TOPK, 4096).reshape((N_PIPE, MICRO, TOKENS, TOPK))
    route_weights = jnp.clip(0.2 + 0.8 * jax.random.uniform(key_list[3], (N_PIPE, MICRO, TOKENS, TOPK), jnp.float32) ** steps_of(key_list[3], (N_PIPE, MICRO, TOKENS, TOPK), ((0, 8), (2, 8)), -0.2, 0.2), 0.2, 1.0)
    picks = jax.vmap(lambda own: jax.random.permutation(own, TOK_DEV))(jax.random.split(key_list[4], N_PIPE * MICRO * N_EXPERT)).reshape((N_PIPE, MICRO, N_EXPERT, TOK_DEV)).astype(jnp.int32)
    w_gate = gaussian(key_list[5], (N_PIPE, EXPERTS, D, FF), D ** -0.5, 0.09375, ((0, 8), (1, 8), (3, 4)))
    w_up = gaussian(key_list[6], (N_PIPE, EXPERTS, D, FF), D ** -0.5, 0.09375, ((0, 8), (1, 8), (3, 4)))
    w_down = gaussian(key_list[7], (N_PIPE, EXPERTS, FF, D), FF ** -0.5, 0.15625, ((0, 8), (1, 8), (2, 4)))
    return dict(tokens=tokens, gains=gains, route_ids=route_ids, route_weights=route_weights, picks=picks, w_gate=w_gate, w_up=w_up, w_down=w_down)


epsilon = 1e-06

def find_slots(ordered_ids, capacity):
    onehot = (ordered_ids[..., None] == jnp.arange(EXPERTS, dtype=jnp.int32)).astype(jnp.int32)
    earlier = jnp.cumsum(onehot, axis=-2) - onehot
    slot_index = lax.optimization_barrier(jnp.sum(earlier * onehot, axis=-1))
    return (slot_index, slot_index < capacity)

def expert_ffn(operands):
    row_block, gate_matrix, up_matrix, down_matrix = operands
    gate_val = jnp.dot(row_block, gate_matrix, preferred_element_type=jnp.float32)
    up_val = jnp.dot(row_block, up_matrix, preferred_element_type=jnp.float32)
    hidden = (jax.nn.silu(gate_val) * up_val).astype(jnp.bfloat16)
    shard_width = FF // N_TENSOR
    summed = jnp.zeros((row_block.shape[0], D), jnp.float32)
    for shard_index in range(N_TENSOR):
        lower = shard_index * shard_width
        partial_sum = jnp.dot(hidden[:, lower:lower + shard_width], down_matrix[lower:lower + shard_width], preferred_element_type=jnp.float32)
        rounded = lax.optimization_barrier(partial_sum.astype(jnp.bfloat16))
        summed = summed + rounded.astype(jnp.float32)
    return summed.astype(jnp.bfloat16)

def moe_section(stream, gain_row, section_ids, section_weights, section_picks, gate_all, up_all, down_all):
    groups = N_EXPERT
    offsets = (jnp.arange(groups, dtype=jnp.int32) * TOK_DEV)[:, None]
    ordered = (section_picks + offsets).astype(jnp.int32).reshape(groups, N_TENSOR, QUARTER)
    stream_f = stream.astype(jnp.float32)
    inv_rms = lax.rsqrt(lax.optimization_barrier(jnp.mean(stream_f * stream_f, axis=1, keepdims=True)) + epsilon)
    normed = (stream_f * inv_rms * gain_row[None, :]).astype(jnp.bfloat16)
    ordered_ids = section_ids[ordered].reshape(groups, N_TENSOR, QUARTER * TOPK)
    ordered_weights = section_weights[ordered].reshape(groups, N_TENSOR, QUARTER * TOPK)
    slot_index, kept_mask = find_slots(ordered_ids, CAP)
    route_tokens = jnp.repeat(ordered, TOPK, axis=2)
    group_index = jnp.arange(groups, dtype=jnp.int32)[:, None, None]
    rank_index = jnp.arange(N_TENSOR, dtype=jnp.int32)[None, :, None]
    position = ((ordered_ids * groups + group_index) * N_TENSOR + rank_index) * CAP + slot_index
    filled = EXPERTS * groups * N_TENSOR * CAP
    target = jnp.where(kept_mask, position, filled).astype(jnp.int32)
    source = jnp.full((filled + 1,), TOKENS, jnp.int32).at[target.reshape(-1)].set(route_tokens.reshape(-1))
    padded = jnp.concatenate([normed, jnp.zeros((1, D), jnp.bfloat16)], axis=0)
    row_block = padded[source[:filled]].reshape(EXPERTS, groups * N_TENSOR * CAP, D)
    results = lax.map(expert_ffn, (row_block, gate_all, up_all, down_all))
    flat_results = jnp.concatenate([results.reshape(filled, D), jnp.zeros((1, D), jnp.bfloat16)], axis=0)
    picked = flat_results[target].astype(jnp.float32)
    weighted = picked * (ordered_weights * kept_mask)[..., None]
    update = lax.optimization_barrier(jnp.sum(weighted.reshape(groups, N_TENSOR, QUARTER, TOPK, D), axis=3))
    stream_new = stream_f.at[ordered.reshape(-1)].add(update.reshape(-1, D))
    return stream_new.astype(jnp.bfloat16)

def reference(tokens, gains, route_ids, route_weights, picks, w_gate, w_up, w_down):
    finished = []
    for micro_index in range(MICRO):
        stream = tokens[micro_index]
        column = []
        for section_index in range(N_PIPE):
            stream = moe_section(stream, gains[section_index], route_ids[section_index, micro_index], route_weights[section_index, micro_index], picks[section_index, micro_index], w_gate[section_index], w_up[section_index], w_down[section_index])
            column.append(stream)
        finished.append(jnp.stack(column))
    return jnp.stack(finished, axis=1)
```

```python
import functools

import jax
import jax.numpy as jnp
import numpy as np
from jax import lax
from jax.experimental import pallas as pl
from jax.experimental.pallas import tpu as pltpu
from jax.sharding import PartitionSpec as P

EPS = 1e-06
CAP = 5
ROWS = 16
BLOCKS = 4
F32 = jnp.float32
BF16 = jnp.bfloat16
MESH = pl.DeviceIdType.MESH


def dot(a, b):
    return jnp.dot(a, b, preferred_element_type=F32)


def kernel(
    sizes,
    tok_hbm,
    wg_hbm,
    wu_hbm,
    wd_hbm,
    gain_ref,
    pm_ref,
    pe_ref,
    cm_ref,
    ce_ref,
    pi_ref,
    pit_ref,
    out_ref,
    w1,
    w2,
    x_buf,
    xs,
    acc,
    part_out,
    part_in,
    first_msg,
    next_msg,
    back_out,
    back_in,
    h_buf,
    w_sem,
    tok_sem,
    a1_send,
    a1_recv,
    a2_send,
    a2_recv,
    b1_send,
    b1_recv,
    b2_send,
    b2_recv,
    h_send,
    h_recv,
):
    stages, ranks, experts, micro, group = sizes
    sets = experts // group
    chunks = micro * sets
    width = h_buf.shape[2]
    narrow = width // BLOCKS
    hidden = w2.shape[1]
    main_rows = group * ROWS
    extra_rows = xs.shape[1] - main_rows
    model = width * ranks
    tok = h_buf.shape[1]
    p = lax.axis_index("pipe")
    t = lax.axis_index("tensor")
    me = lax.axis_index("expert")
    my_set = lax.rem(me, sets)
    my_place = me // sets

    def peer(i):
        return lax.rem(t + i, ranks)

    def other(i):
        return lax.rem(me + i, experts)

    def remote(src, dst, send, recv, where):
        return pltpu.make_async_remote_copy(
            src_ref=src, dst_ref=dst, send_sem=send, recv_sem=recv, device_id=where, device_id_type=MESH
        )

    loads = []
    for f in range(ranks):
        rows = pl.ds(f * width, width)
        loads.append(pltpu.make_async_copy(wg_hbm.at[rows, :], w1.at[f, :, pl.ds(0, hidden)], w_sem.at[f]))
        loads.append(pltpu.make_async_copy(wu_hbm.at[rows, :], w1.at[f, :, pl.ds(hidden, hidden)], w_sem.at[ranks + f]))
        loads.append(pltpu.make_async_copy(wd_hbm.at[:, rows], w2.at[f], w_sem.at[2 * ranks + f]))
    slice_start = pl.multiple_of(t * width, 128)
    tok_load = pltpu.make_async_copy(tok_hbm.at[:, :, pl.ds(slice_start, width)], h_buf, tok_sem)

    @pl.when(p == 0)
    def _():
        tok_load.start()

    for load in loads:
        load.start()

    barrier = pltpu.get_barrier_semaphore()
    for i in range(1, ranks):
        pl.semaphore_signal(barrier, inc=1, device_id={"tensor": peer(i)}, device_id_type=MESH)
    for i in range(1, experts):
        pl.semaphore_signal(barrier, inc=1, device_id={"expert": other(i)}, device_id_type=MESH)

    @pl.when(p < stages - 1)
    def _():
        for e in range(experts):
            pl.semaphore_signal(barrier, inc=1, device_id={"pipe": p + 1, "expert": e}, device_id_type=MESH)

    @pl.when(p > 0)
    def _():
        for e in range(experts):
            pl.semaphore_signal(barrier, inc=1, device_id={"pipe": p - 1, "expert": e}, device_id_type=MESH)

    ahead = jnp.where(p < stages - 1, experts, 0)
    behind = jnp.where(p > 0, experts, 0)
    pl.semaphore_wait(barrier, ranks - 1 + experts - 1 + ahead + behind)

    def fill_messages(msg, which, m, stream):
        main = dot(pm_ref[which, m], stream).astype(BF16)
        stacked = jnp.concatenate([stream[:, b * narrow : (b + 1) * narrow] for b in range(BLOCKS)], axis=0)
        extra = dot(pe_ref[which, m], stacked).astype(BF16)
        for e in range(experts):
            msg[m, e, :, pl.ds(0, width)] = main[e * ROWS : (e + 1) * ROWS]
            msg[m, e, :, pl.ds(width, narrow)] = extra[e * ROWS : (e + 1) * ROWS]

    def first_copy(m, i):
        e = other(i)
        c = m * sets + my_set
        return remote(
            first_msg.at[m, e],
            x_buf.at[c, t, my_place],
            a1_send.at[0, m, e],
            a1_recv.at[c, my_place],
            {"expert": e},
        )

    def next_copy(m, e):
        c = m * sets + my_set
        return remote(
            next_msg.at[m, e],
            x_buf.at[c, t, my_place],
            a1_send.at[1, m, e],
            a1_recv.at[c, my_place],
            {"pipe": p + 1, "expert": e},
        )

    def stream_copy(m):
        return remote(out_ref.at[m], h_buf.at[m], h_send.at[m], h_recv.at[m], {"pipe": p + 1})

    def relay_copy(c, j, i):
        return remote(
            x_buf.at[c, t, j], x_buf.at[c, t, j], a2_send.at[c, j, i - 1], a2_recv.at[c, t, j], {"tensor": peer(i)}
        )

    def part_copy(c, i):
        return remote(
            part_out.at[c, i - 1], part_in.at[c, t], b1_send.at[c, i - 1], b1_recv.at[c, t], {"tensor": peer(i)}
        )

    def back_copy(c, j):
        m = c // sets
        g = j * sets + lax.rem(c, sets)
        return remote(back_out.at[c, j], back_in.at[m, me], b2_send.at[c, j], b2_recv.at[m, me], {"expert": g})

    @pl.when(p == 0)
    def _():
        tok_load.wait()
        for m in range(micro):
            fill_messages(first_msg, 0, m, h_buf[m])
            for i in range(1, experts):
                first_copy(m, i).start()
            x_buf[m * sets + my_set, t, my_place] = first_msg[m, me]

    for load in loads:
        load.wait()

    def relay(c):
        for j in range(group):
            g = j * sets + lax.rem(c, sets)

            @pl.when((p > 0) | (g != me))
            def _():
                remote(
                    first_msg.at[0, 0], x_buf.at[c, t, j], a1_send.at[0, 0, 0], a1_recv.at[c, j], {"expert": other(1)}
                ).wait_recv()

            for i in (2, 1, 3):
                relay_copy(c, j, i).start()

    def experts_work(c):
        total = None
        squares = None
        for i in (0, 1, 3, 2):
            f = peer(i)
            if i > 0:
                for j in range(group):
                    remote(
                        x_buf.at[c, f, j], x_buf.at[c, f, j], a2_send.at[c, j, i - 1], a2_recv.at[c, f, j], {"tensor": f}
                    ).wait_recv()
            gain = gain_ref[f]
            main = x_buf[c, f, :, :, pl.ds(0, width)].reshape(main_rows, width).astype(F32)
            xs[f, pl.ds(0, main_rows), :] = (main * gain).astype(BF16)
            packed = x_buf[c, f, :, :, pl.ds(width, narrow)].reshape(main_rows, narrow)
            extra = dot(pi_ref[...], packed)
            extra_sq = jnp.zeros((extra_rows, 1), F32)
            for b in range(BLOCKS):
                block = extra[b * extra_rows : (b + 1) * extra_rows]
                cols = slice(b * narrow, (b + 1) * narrow)
                extra_sq = extra_sq + jnp.sum(block * block, axis=1, keepdims=True)
                xs[f, pl.ds(main_rows, extra_rows), pl.ds(b * narrow, narrow)] = (block * gain[:, cols]).astype(BF16)
            sq = jnp.concatenate([jnp.sum(main * main, axis=1, keepdims=True), extra_sq], axis=0)
            squares = sq if squares is None else squares + sq
            if i == 0:
                acc[...] = dot(xs[f], w1[f])
            else:
                acc[...] += dot(xs[f], w1[f])
        inv = lax.rsqrt(squares * (1.0 / model) + EPS)
        gate = acc[:, pl.ds(0, hidden)] * inv
        up = acc[:, pl.ds(hidden, hidden)] * inv
        act = (gate / (1.0 + jnp.exp(-gate)) * up).astype(BF16)
        for i in (2, 1, 3, 0):
            part = dot(act, w2[peer(i)]).astype(BF16)
            if i == 0:
                part_in[c, t] = part
            else:
                part_out[c, i - 1] = part
                part_copy(c, i).start()

    def give_back(c):
        m = c // sets
        for i in range(1, ranks):
            f = peer(i)
            remote(part_out.at[c, i - 1], part_in.at[c, f], b1_send.at[c, i - 1], b1_recv.at[c, f], {"tensor": f}).wait_recv()
        total = part_in[c, 0].astype(F32)
        for q in range(1, ranks):
            total = total + part_in[c, q].astype(F32)
        total = total.astype(BF16)
        extra = total[main_rows:]
        stacked = jnp.concatenate([extra[:, b * narrow : (b + 1) * narrow] for b in range(BLOCKS)], axis=0)
        packed = dot(pit_ref[...], stacked).astype(BF16)
        for j in range(group):
            back_out[c, j, :, pl.ds(0, width)] = total[j * ROWS : (j + 1) * ROWS]
            back_out[c, j, :, pl.ds(width, narrow)] = packed[j * ROWS : (j + 1) * ROWS]
        for j in range(group):
            g = j * sets + lax.rem(c, sets)

            @pl.when(g != me)
            def _():
                back_copy(c, j).start()

            @pl.when(g == me)
            def _():
                back_in[m, me] = back_out[c, j]

    def combine(c):
        m = c // sets

        @pl.when(lax.rem(c, sets) == my_set)
        def _():
            for i in range(1, experts):
                e = other(i)
                remote(back_out.at[c, 0], back_in.at[m, e], b2_send.at[c, 0], b2_recv.at[m, e], {"expert": e}).wait_recv()

            @pl.when(p > 0)
            def _():
                remote(out_ref.at[m], h_buf.at[m], h_send.at[m], h_recv.at[m], {"expert": other(1)}).wait_recv()

            main = back_in[m, :, :, pl.ds(0, width)].reshape(experts * ROWS, width)
            packed = back_in[m, :, :, pl.ds(width, narrow)].reshape(experts * ROWS, narrow)
            wide = dot(cm_ref[m], main)
            update = wide[:tok] + wide[tok:]
            thin = dot(ce_ref[m], packed)
            thin = thin[: BLOCKS * tok] + thin[BLOCKS * tok :]
            spread = jnp.concatenate([thin[b * tok : (b + 1) * tok] for b in range(BLOCKS)], axis=1)
            fresh = (h_buf[m].astype(F32) + update + spread).astype(BF16)
            out_ref[m] = fresh

            @pl.when(p < stages - 1)
            def _():
                fill_messages(next_msg, 1, m, fresh)
                for e in range(experts):
                    next_copy(m, e).start()
                stream_copy(m).start()

    def step(s, carry):
        @pl.when(s < chunks)
        def _():
            relay(s)

        @pl.when(s > 0)
        def _():
            give_back(s - 1)

        @pl.when(s < chunks)
        def _():
            experts_work(s)

        @pl.when(s > 0)
        def _():
            combine(s - 1)

        return carry

    lax.fori_loop(0, chunks + 1, step, 0)

    @pl.when(p == 0)
    def _():
        for m in range(micro):
            for i in range(1, experts):
                first_copy(m, i).wait_send()

    @pl.when(p < stages - 1)
    def _():
        for m in range(micro):
            for e in range(experts):
                next_copy(m, e).wait_send()
            stream_copy(m).wait_send()

    def drain(c, carry):
        for j in range(group):
            for i in range(1, ranks):
                relay_copy(c, j, i).wait_send()
            g = j * sets + lax.rem(c, sets)

            @pl.when(g != me)
            def _():
                back_copy(c, j).wait_send()

        for i in range(1, ranks):
            part_copy(c, i).wait_send()
        return carry

    lax.fori_loop(0, chunks, drain, 0)


def positions(ids, weights, order, experts, ranks):
    tok = order.shape[-1]
    index = jnp.arange(tok, dtype=jnp.int32)
    rank = jnp.sum(jnp.where(order[:, :, None] == index[None, None, :], index[None, :, None], 0), axis=1)
    quarter = rank // (tok // ranks)
    names = ids[..., None] == jnp.arange(experts, dtype=jnp.int32)
    named = jnp.any(names, axis=2)
    weight = jnp.sum(jnp.where(names, weights[..., None], 0.0), axis=2)
    before = (quarter[:, :, None] == quarter[:, None, :]) & (rank[:, None, :] < rank[:, :, None])
    slot = jnp.sum((before[..., None] & named[:, None]).astype(jnp.int32), axis=2)
    kept = named & (slot < CAP)
    return jnp.where(kept, quarter[..., None] * CAP + slot, -1), weight


def placing(pos):
    micro, tok, experts = pos.shape
    by_expert = jnp.swapaxes(pos, 1, 2)[:, :, None, :]
    main = by_expert == jnp.arange(ROWS, dtype=jnp.int32)[None, None, :, None]
    k = jnp.arange(BLOCKS, dtype=jnp.int32)
    extra = by_expert[:, :, None, :, None, :] == (ROWS + k)[None, None, None, :, None, None]
    same = k[:, None] == k[None, :]
    extra = extra & same[None, None, :, None, :, None]
    main = main.reshape(micro, experts * ROWS, tok).astype(BF16)
    extra = extra.reshape(micro, experts * ROWS, BLOCKS * tok).astype(BF16)
    return main, extra


def gathering(pos, weight):
    micro, tok, experts = pos.shape
    high = weight.astype(BF16).astype(F32)
    both = jnp.stack([high, weight - high], axis=1)[..., None]
    main = jnp.where((pos[..., None] == jnp.arange(ROWS, dtype=jnp.int32))[:, None], both, 0.0)
    k = jnp.arange(BLOCKS, dtype=jnp.int32)
    extra = jnp.where((pos[..., None] == ROWS + k)[:, None], both, 0.0)
    same = k[:, None] == k[None, :]
    extra = jnp.where(same[None, None, :, None, None, :, None], extra[:, :, None, :, :, None, :], 0.0)
    main = main.reshape(micro, 2 * tok, experts * ROWS).astype(BF16)
    extra = extra.reshape(micro, 2 * BLOCKS * tok, experts * ROWS).astype(BF16)
    return main, extra


def local(sizes, tokens, gains, route_ids, route_weights, picks, w_gate, w_up, w_down):
    stages, ranks, experts, micro, group = sizes
    tok, model = tokens.shape[1:]
    width = model // ranks
    narrow = width // BLOCKS
    wide = width + narrow
    hidden = w_gate.shape[3]
    chunks = micro * (experts // group)
    main_rows = group * ROWS
    extra_rows = max(ROWS, BLOCKS * group)
    rows = main_rows + extra_rows

    pos, weight = positions(route_ids[0], route_weights[0], picks[0, :, 0], experts, ranks)
    following = lax.ppermute(pos, "pipe", [(i + 1, i) for i in range(stages - 1)])
    pm, pe = placing(jnp.concatenate([pos, following], axis=0))
    pm = pm.reshape(2, micro, *pm.shape[1:])
    pe = pe.reshape(2, micro, *pe.shape[1:])
    cm, ce = gathering(pos, weight)

    permute = np.zeros((BLOCKS, extra_rows, group, BLOCKS, BLOCKS), np.float32)
    for b in range(BLOCKS):
        for j in range(group):
            for k in range(BLOCKS):
                permute[b, j * BLOCKS + k, j, b, k] = 1.0
    permute = permute.reshape(BLOCKS * extra_rows, main_rows)
    pi = jnp.asarray(permute, BF16)
    pit = jnp.asarray(permute.T.copy(), BF16)

    vmem = pl.BlockSpec(memory_space=pltpu.VMEM)
    hbm = pl.BlockSpec(memory_space=pl.ANY)
    dma = pltpu.SemaphoreType.DMA
    out = pl.pallas_call(
        functools.partial(kernel, sizes),
        out_shape=jax.ShapeDtypeStruct((micro, tok, width), BF16),
        in_specs=[hbm] * 4 + [vmem] * 7,
        out_specs=vmem,
        scratch_shapes=[
            pltpu.VMEM((ranks, width, 2 * hidden), BF16),
            pltpu.VMEM((ranks, hidden, width), BF16),
            pltpu.VMEM((chunks, ranks, group, ROWS, wide), BF16),
            pltpu.VMEM((ranks, rows, width), BF16),
            pltpu.VMEM((rows, 2 * hidden), F32),
            pltpu.VMEM((chunks, ranks - 1, rows, width), BF16),
            pltpu.VMEM((chunks, ranks, rows, width), BF16),
            pltpu.VMEM((micro, experts, ROWS, wide), BF16),
            pltpu.VMEM((micro, experts, ROWS, wide), BF16),
            pltpu.VMEM((chunks, group, ROWS, wide), BF16),
            pltpu.VMEM((micro, experts, ROWS, wide), BF16),
            pltpu.VMEM((micro, tok, width), BF16),
            dma((3 * ranks,)),
            dma,
            dma((2, micro, experts)),
            dma((chunks, group)),
            dma((chunks, group, ranks - 1)),
            dma((chunks, ranks, group)),
            dma((chunks, ranks - 1)),
            dma((chunks, ranks)),
            dma((chunks, group)),
            dma((micro, experts)),
            dma((micro,)),
            dma((micro,)),
        ],
        compiler_params=pltpu.CompilerParams(
            collective_id=0, has_side_effects=True, vmem_limit_bytes=60_000_000
        ),
    )(
        tokens,
        w_gate[0, 0],
        w_up[0, 0],
        w_down[0, 0],
        gains.reshape(ranks, 1, width),
        pm,
        pe,
        cm,
        ce,
        pi,
        pit,
    )
    return out[None]


def solution(mesh, group=2):
    experts = mesh.shape["expert"]
    sizes = (mesh.shape["pipe"], mesh.shape["tensor"], experts, 2, min(group, experts))
    return jax.shard_map(
        functools.partial(local, sizes),
        mesh=mesh,
        in_specs=(
            P(None, "expert", None),
            P("pipe", None),
            P("pipe", None, "expert", None),
            P("pipe", None, "expert", None),
            P("pipe", None, "expert", None),
            P("pipe", "expert", None, "tensor"),
            P("pipe", "expert", None, "tensor"),
            P("pipe", "expert", "tensor", None),
        ),
        out_specs=P("pipe", None, "expert", "tensor"),
        check_vma=False,
    )
```

```python
import functools

import jax
import jax.numpy as jnp
import numpy as np
from jax import lax
from jax.experimental import pallas as pl
from jax.experimental.pallas import tpu as pltpu
from jax.sharding import PartitionSpec as P

EPS = 1e-06
CAP = 5
ROWS = 16
BLOCKS = 4
F32 = jnp.float32
BF16 = jnp.bfloat16
MESH = pl.DeviceIdType.MESH


def dot(a, b):
    return jnp.dot(a, b, preferred_element_type=F32)


def kernel(
    sizes,
    tok_hbm,
    wg_hbm,
    wu_hbm,
    wd_hbm,
    gain_ref,
    ids_ref,
    idst_ref,
    wt_ref,
    row_ref,
    col_ref,
    pi_ref,
    pit_ref,
    out_ref,
    pm_ref,
    pe_ref,
    cm_ref,
    ce_ref,
    post,
    pos_tok,
    w1,
    w2,
    x_buf,
    xs,
    acc,
    part_out,
    part_in,
    first_msg,
    next_msg,
    back_out,
    back_in,
    h_buf,
    w_sem,
    tok_sem,
    a1_send,
    a1_recv,
    a2_send,
    a2_recv,
    b1_send,
    b1_recv,
    b2_send,
    b2_recv,
    h_send,
    h_recv,
    post_send,
    post_recv,
):
    stages, ranks, experts, micro, group = sizes
    sets = experts // group
    chunks = micro * sets
    width = h_buf.shape[2]
    narrow = width // BLOCKS
    hidden = w2.shape[1]
    main_rows = group * ROWS
    extra_rows = xs.shape[1] - main_rows
    model = width * ranks
    tok = h_buf.shape[1]
    p = lax.axis_index("pipe")
    t = lax.axis_index("tensor")
    me = lax.axis_index("expert")
    my_set = lax.rem(me, sets)
    my_place = me // sets

    def peer(i):
        return lax.rem(t + i, ranks)

    def other(i):
        return lax.rem(me + i, experts)

    order = sorted(range(experts), key=lambda i: -min(i // 2, (experts - 1 - i) // 2 + 1 if i > 1 else 0))

    def other_chip(i):
        return lax.rem(me - lax.rem(me, 2) + i, experts)

    def remote(src, dst, send, recv, where):
        return pltpu.make_async_remote_copy(
            src_ref=src, dst_ref=dst, send_sem=send, recv_sem=recv, device_id=where, device_id_type=MESH
        )

    loads = []
    for f in range(ranks):
        rows = pl.ds(f * width, width)
        loads.append(pltpu.make_async_copy(wg_hbm.at[rows, :], w1.at[f, :, pl.ds(0, hidden)], w_sem.at[f]))
        loads.append(pltpu.make_async_copy(wu_hbm.at[rows, :], w1.at[f, :, pl.ds(hidden, hidden)], w_sem.at[ranks + f]))
        loads.append(pltpu.make_async_copy(wd_hbm.at[:, rows], w2.at[f], w_sem.at[2 * ranks + f]))
    slice_start = pl.multiple_of(t * width, 128)
    tok_load = pltpu.make_async_copy(tok_hbm.at[:, :, pl.ds(slice_start, width)], h_buf, tok_sem)

    @pl.when(p == 0)
    def _():
        tok_load.start()

    for load in loads:
        load.start()

    def count(shape, dim):
        return lax.broadcasted_iota(jnp.int32, shape, dim)

    def slots(m):
        across, down = count((tok, tok), 1), count((tok, tok), 0)
        rank_row = jnp.sum(jnp.where(col_ref[m] == across, down.astype(F32), 0.0), axis=0, keepdims=True)
        rank_col = jnp.sum(jnp.where(row_ref[m] == down, across.astype(F32), 0.0), axis=1, keepdims=True)
        part_row = jnp.floor(rank_row * (ranks / tok))
        part_col = jnp.floor(rank_col * (ranks / tok))
        same = jnp.where(part_row == part_col, 1.0, 0.0)
        before_t = (jnp.where(rank_col < rank_row, 1.0, 0.0) * same).astype(BF16)
        before = (jnp.where(rank_row < rank_col, 1.0, 0.0) * same).astype(BF16)
        e_down, e_across = count((experts, tok), 0), count((tok, experts), 1)
        ids, idst = ids_ref[m], idst_ref[m]
        named_t = jnp.where((idst[0:1] == e_down) | (idst[1:2] == e_down), 1.0, 0.0)
        named = jnp.where((ids[:, 0:1] == e_across) | (ids[:, 1:2] == e_across), 1.0, 0.0)
        slot_t = dot(named_t.astype(BF16), before_t)
        slot = dot(before, named.astype(BF16))
        post[0, m] = jnp.where((named_t > 0.0) & (slot_t < CAP), part_row * CAP + slot_t, -1.0)
        pos_tok[m] = jnp.where((named > 0.0) & (slot < CAP), part_col * CAP + slot, -1.0)

    def place(which, m):
        pos = post[which, m]
        four = jnp.concatenate([pos] * BLOCKS, axis=1)
        plain = count((ROWS, tok), 0).astype(F32)
        down, across = count((ROWS, BLOCKS * tok), 0), count((ROWS, BLOCKS * tok), 1)
        shift = tok.bit_length() - 1
        own = lax.shift_right_logical(across, shift) == lax.shift_right_logical(down, 2)
        slot = jnp.where(own, (ROWS + (down & 3)).astype(F32), -2.0)
        for e in range(experts):
            rows = pl.ds(e * ROWS, ROWS)
            pm_ref[which, m, rows, :] = jnp.where(pos[e : e + 1] == plain, 1.0, 0.0).astype(BF16)
            pe_ref[which, m, rows, :] = jnp.where(four[e : e + 1] == slot, 1.0, 0.0).astype(BF16)

    def gather(m):
        lanes = experts * ROWS
        e_across = count((tok, experts), 1)
        ids, wt = ids_ref[m], wt_ref[m]
        weight = jnp.where(ids[:, 0:1] == e_across, wt[:, 0:1], 0.0)
        weight = weight + jnp.where(ids[:, 1:2] == e_across, wt[:, 1:2], 0.0)
        high = weight.astype(BF16)
        low = (weight - high.astype(F32)).astype(BF16)
        block = lax.shift_right_logical(count((experts, lanes), 1), 4) == count((experts, lanes), 0)
        widen = jnp.where(block, 1.0, 0.0).astype(BF16)
        pos = dot(pos_tok[m].astype(BF16), widen)
        lane = count((tok, lanes), 1)
        inside = lane & (ROWS - 1)
        plain = inside.astype(F32)
        tail = (ROWS + (lane & 3)).astype(F32)
        for n, half in enumerate((high, low)):
            value = dot(half, widen)
            cm_ref[m, pl.ds(n * tok, tok), :] = jnp.where(pos == plain, value, 0.0).astype(BF16)
            for b in range(BLOCKS):
                mine = (pos == tail) & (lax.shift_right_logical(inside, 2) == b)
                ce_ref[m, pl.ds((n * BLOCKS + b) * tok, tok), :] = jnp.where(mine, value, 0.0).astype(BF16)

    for m in range(micro):
        slots(m)

    barrier = pltpu.get_barrier_semaphore()
    for i in range(1, ranks):
        pl.semaphore_signal(barrier, inc=1, device_id={"tensor": peer(i)}, device_id_type=MESH)
    for i in range(1, experts):
        pl.semaphore_signal(barrier, inc=1, device_id={"expert": other(i)}, device_id_type=MESH)

    @pl.when(p < stages - 1)
    def _():
        for e in range(experts):
            pl.semaphore_signal(barrier, inc=1, device_id={"pipe": p + 1, "expert": e}, device_id_type=MESH)

    @pl.when(p > 0)
    def _():
        for e in range(experts):
            pl.semaphore_signal(barrier, inc=1, device_id={"pipe": p - 1, "expert": e}, device_id_type=MESH)

    ahead = jnp.where(p < stages - 1, experts, 0)
    behind = jnp.where(p > 0, experts, 0)
    pl.semaphore_wait(barrier, ranks - 1 + experts - 1 + ahead + behind)

    def fill_messages(msg, which, m, stream):
        main = dot(pm_ref[which, m], stream).astype(BF16)
        stacked = jnp.concatenate([stream[:, b * narrow : (b + 1) * narrow] for b in range(BLOCKS)], axis=0)
        extra = dot(pe_ref[which, m], stacked).astype(BF16)
        for e in range(experts):
            msg[m, e, :, pl.ds(0, width)] = main[e * ROWS : (e + 1) * ROWS]
            msg[m, e, :, pl.ds(width, narrow)] = extra[e * ROWS : (e + 1) * ROWS]

    def first_copy(m, i):
        e = other(i)
        c = m * sets + my_set
        return remote(
            first_msg.at[m, e],
            x_buf.at[c, t, my_place],
            a1_send.at[0, m, e],
            a1_recv.at[c, my_place],
            {"expert": e},
        )

    def next_copy(m, e):
        c = m * sets + my_set
        return remote(
            next_msg.at[m, e],
            x_buf.at[c, t, my_place],
            a1_send.at[1, m, e],
            a1_recv.at[c, my_place],
            {"pipe": p + 1, "expert": e},
        )

    def post_copy():
        return remote(post.at[0], post.at[1], post_send, post_recv, {"pipe": p - 1})

    def stream_copy(m):
        return remote(out_ref.at[m], h_buf.at[m], h_send.at[m], h_recv.at[m], {"pipe": p + 1})

    def relay_copy(c, j, i):
        return remote(
            x_buf.at[c, t, j], x_buf.at[c, t, j], a2_send.at[c, j, i - 1], a2_recv.at[c, t, j], {"tensor": peer(i)}
        )

    def part_copy(c, i):
        return remote(
            part_out.at[c, i - 1], part_in.at[c, t], b1_send.at[c, i - 1], b1_recv.at[c, t], {"tensor": peer(i)}
        )

    def back_copy(c, j):
        m = c // sets
        g = j * sets + lax.rem(c, sets)
        return remote(back_out.at[c, j], back_in.at[m, me], b2_send.at[c, j], b2_recv.at[m, me], {"expert": g})

    def relay(c):
        near = lax.rem((me + experts - lax.rem(c, sets)) // 2, experts // 2) * 2 // sets
        for n in range(group):
            j = lax.rem(near + n, group)
            g = j * sets + lax.rem(c, sets)

            @pl.when((p > 0) | (g != me))
            def _():
                remote(
                    first_msg.at[0, 0], x_buf.at[c, t, j], a1_send.at[0, 0, 0], a1_recv.at[c, j], {"expert": other(1)}
                ).wait_recv()

            for i in (2, 1, 3):
                relay_copy(c, j, i).start()

    def experts_work(c):
        total = None
        squares = None
        for i in (0, 1, 3, 2):
            f = peer(i)
            if i > 0:
                for j in range(group):
                    remote(
                        x_buf.at[c, f, j], x_buf.at[c, f, j], a2_send.at[c, j, i - 1], a2_recv.at[c, f, j], {"tensor": f}
                    ).wait_recv()
            gain = gain_ref[f]
            main = x_buf[c, f, :, :, pl.ds(0, width)].reshape(main_rows, width).astype(F32)
            xs[f, pl.ds(0, main_rows), :] = (main * gain).astype(BF16)
            packed = x_buf[c, f, :, :, pl.ds(width, narrow)].reshape(main_rows, narrow)
            extra = dot(pi_ref[...], packed)
            extra_sq = jnp.zeros((extra_rows, 1), F32)
            for b in range(BLOCKS):
                block = extra[b * extra_rows : (b + 1) * extra_rows]
                cols = slice(b * narrow, (b + 1) * narrow)
                extra_sq = extra_sq + jnp.sum(block * block, axis=1, keepdims=True)
                xs[f, pl.ds(main_rows, extra_rows), pl.ds(b * narrow, narrow)] = (block * gain[:, cols]).astype(BF16)
            sq = jnp.concatenate([jnp.sum(main * main, axis=1, keepdims=True), extra_sq], axis=0)
            squares = sq if squares is None else squares + sq
            if i == 0:
                acc[...] = dot(xs[f], w1[f])
            else:
                acc[...] += dot(xs[f], w1[f])
        inv = lax.rsqrt(squares * (1.0 / model) + EPS)
        gate = acc[:, pl.ds(0, hidden)] * inv
        up = acc[:, pl.ds(hidden, hidden)] * inv
        act = (gate / (1.0 + jnp.exp(-gate)) * up).astype(BF16)
        for i in (2, 1, 3, 0):
            part = dot(act, w2[peer(i)]).astype(BF16)
            extra = part[main_rows:]
            stacked = jnp.concatenate([extra[:, b * narrow : (b + 1) * narrow] for b in range(BLOCKS)], axis=0)
            packed = dot(pit_ref[...], stacked).astype(BF16)
            wide = jnp.concatenate([part[:main_rows], packed], axis=1).reshape(group, ROWS, width + narrow)
            if i == 0:
                part_in[c, t] = wide
            else:
                part_out[c, i - 1] = wide
                part_copy(c, i).start()

    def give_back(c):
        m = c // sets
        for i in range(1, ranks):
            f = peer(i)
            remote(part_out.at[c, i - 1], part_in.at[c, f], b1_send.at[c, i - 1], b1_recv.at[c, f], {"tensor": f}).wait_recv()
        total = part_in[c, 0].astype(F32)
        for q in range(1, ranks):
            total = total + part_in[c, q].astype(F32)
        back_out[c] = total.astype(BF16)
        for j in range(group):
            g = j * sets + lax.rem(c, sets)

            @pl.when(g != me)
            def _():
                back_copy(c, j).start()

            @pl.when(g == me)
            def _():
                back_in[m, me] = back_out[c, j]

    def combine(c):
        m = c // sets

        @pl.when(lax.rem(c, sets) == my_set)
        def _():
            for i in range(1, experts):
                e = other(i)
                remote(back_out.at[c, 0], back_in.at[m, e], b2_send.at[c, 0], b2_recv.at[m, e], {"expert": e}).wait_recv()

            @pl.when(p > 0)
            def _():
                remote(out_ref.at[m], h_buf.at[m], h_send.at[m], h_recv.at[m], {"expert": other(1)}).wait_recv()

            main = back_in[m, :, :, pl.ds(0, width)].reshape(experts * ROWS, width)
            packed = back_in[m, :, :, pl.ds(width, narrow)].reshape(experts * ROWS, narrow)
            wide = dot(cm_ref[m], main)
            update = wide[:tok] + wide[tok:]
            thin = dot(ce_ref[m], packed)
            thin = thin[: BLOCKS * tok] + thin[BLOCKS * tok :]
            spread = jnp.concatenate([thin[b * tok : (b + 1) * tok] for b in range(BLOCKS)], axis=1)
            fresh = (h_buf[m].astype(F32) + update + spread).astype(BF16)
            out_ref[m] = fresh

            @pl.when(p < stages - 1)
            def _():
                fill_messages(next_msg, 1, m, fresh)
                for i in order:
                    next_copy(m, other_chip(i)).start()
                stream_copy(m).start()

    @pl.when(p > 0)
    def _():
        post_copy().start()

    @pl.when(p == 0)
    def _():
        tok_load.wait()
        for m in range(micro):
            place(0, m)
            fill_messages(first_msg, 0, m, h_buf[m])
            for i in range(1, experts):
                first_copy(m, i).start()
            x_buf[m * sets + my_set, t, my_place] = first_msg[m, me]
        relay(0)

    for m in range(micro):
        gather(m)

    @pl.when(p < stages - 1)
    def _():
        remote(post.at[0], post.at[1], post_send, post_recv, {"expert": other(1)}).wait_recv()
        for m in range(micro):
            place(1, m)

    for load in loads:
        load.wait()

    def step(s, carry):
        @pl.when((s < chunks) & ((s > 0) | (p > 0)))
        def _():
            relay(s)

        @pl.when(s > 0)
        def _():
            give_back(s - 1)

        @pl.when(s < chunks)
        def _():
            experts_work(s)

        @pl.when(s > 0)
        def _():
            combine(s - 1)

        return carry

    lax.fori_loop(0, chunks + 1, step, 0)

    @pl.when(p > 0)
    def _():
        post_copy().wait_send()

    @pl.when(p == 0)
    def _():
        for m in range(micro):
            for i in range(1, experts):
                first_copy(m, i).wait_send()

    @pl.when(p < stages - 1)
    def _():
        for m in range(micro):
            for e in range(experts):
                next_copy(m, e).wait_send()
            stream_copy(m).wait_send()

    def drain(c, carry):
        for j in range(group):
            for i in range(1, ranks):
                relay_copy(c, j, i).wait_send()
            g = j * sets + lax.rem(c, sets)

            @pl.when(g != me)
            def _():
                back_copy(c, j).wait_send()

        for i in range(1, ranks):
            part_copy(c, i).wait_send()
        return carry

    lax.fori_loop(0, chunks, drain, 0)


def local(sizes, tokens, gains, route_ids, route_weights, picks, w_gate, w_up, w_down):
    stages, ranks, experts, micro, group = sizes
    tok, model = tokens.shape[1:]
    width = model // ranks
    narrow = width // BLOCKS
    wide = width + narrow
    hidden = w_gate.shape[3]
    chunks = micro * (experts // group)
    main_rows = group * ROWS
    extra_rows = max(ROWS, BLOCKS * group)
    rows = main_rows + extra_rows

    permute = np.zeros((BLOCKS, extra_rows, group, BLOCKS, BLOCKS), np.float32)
    for b in range(BLOCKS):
        for j in range(group):
            for k in range(BLOCKS):
                permute[b, j * BLOCKS + k, j, b, k] = 1.0
    permute = permute.reshape(BLOCKS * extra_rows, main_rows)
    pi = jnp.asarray(permute, BF16)
    pit = jnp.asarray(permute.T.copy(), BF16)

    vmem = pl.BlockSpec(memory_space=pltpu.VMEM)
    hbm = pl.BlockSpec(memory_space=pl.ANY)
    dma = pltpu.SemaphoreType.DMA
    out = pl.pallas_call(
        functools.partial(kernel, sizes),
        out_shape=jax.ShapeDtypeStruct((micro, tok, width), BF16),
        in_specs=[hbm] * 4 + [vmem] * 8,
        out_specs=vmem,
        scratch_shapes=[
            pltpu.VMEM((2, micro, experts * ROWS, tok), BF16),
            pltpu.VMEM((2, micro, experts * ROWS, BLOCKS * tok), BF16),
            pltpu.VMEM((micro, 2 * tok, experts * ROWS), BF16),
            pltpu.VMEM((micro, 2 * BLOCKS * tok, experts * ROWS), BF16),
            pltpu.VMEM((2, micro, experts, tok), F32),
            pltpu.VMEM((micro, tok, experts), F32),
            pltpu.VMEM((ranks, width, 2 * hidden), BF16),
            pltpu.VMEM((ranks, hidden, width), BF16),
            pltpu.VMEM((chunks, ranks, group, ROWS, wide), BF16),
            pltpu.VMEM((ranks, rows, width), BF16),
            pltpu.VMEM((rows, 2 * hidden), F32),
            pltpu.VMEM((chunks, ranks - 1, group, ROWS, wide), BF16),
            pltpu.VMEM((chunks, ranks, group, ROWS, wide), BF16),
            pltpu.VMEM((micro, experts, ROWS, wide), BF16),
            pltpu.VMEM((micro, experts, ROWS, wide), BF16),
            pltpu.VMEM((chunks, group, ROWS, wide), BF16),
            pltpu.VMEM((micro, experts, ROWS, wide), BF16),
            pltpu.VMEM((micro, tok, width), BF16),
            dma((3 * ranks,)),
            dma,
            dma((2, micro, experts)),
            dma((chunks, group)),
            dma((chunks, group, ranks - 1)),
            dma((chunks, ranks, group)),
            dma((chunks, ranks - 1)),
            dma((chunks, ranks)),
            dma((chunks, group)),
            dma((micro, experts)),
            dma((micro,)),
            dma((micro,)),
            dma,
            dma,
        ],
        compiler_params=pltpu.CompilerParams(
            collective_id=0, has_side_effects=True, vmem_limit_bytes=60_000_000
        ),
    )(
        tokens,
        w_gate[0, 0],
        w_up[0, 0],
        w_down[0, 0],
        gains.reshape(ranks, 1, width),
        route_ids[0],
        jnp.swapaxes(route_ids[0], 1, 2),
        route_weights[0],
        picks[0],
        jnp.swapaxes(picks[0], 1, 2),
        pi,
        pit,
    )
    return out[None]


def solution(mesh, group=2):
    experts = mesh.shape["expert"]
    sizes = (mesh.shape["pipe"], mesh.shape["tensor"], experts, 2, min(group, experts))
    return jax.shard_map(
        functools.partial(local, sizes),
        mesh=mesh,
        in_specs=(
            P(None, "expert", None),
            P("pipe", None),
            P("pipe", None, "expert", None),
            P("pipe", None, "expert", None),
            P("pipe", None, "expert", None),
            P("pipe", "expert", None, "tensor"),
            P("pipe", "expert", None, "tensor"),
            P("pipe", "expert", "tensor", None),
        ),
        out_specs=P("pipe", None, "expert", "tensor"),
        check_vma=False,
    )
```

```python
import functools

import jax
import jax.numpy as jnp
import numpy as np
from jax import lax
from jax.experimental import pallas as pl
from jax.experimental.pallas import tpu as pltpu
from jax.sharding import PartitionSpec as P

EPS = 1e-06
CAP = 5
ROWS = 16
BLOCKS = 4
F32 = jnp.float32
BF16 = jnp.bfloat16
MESH = pl.DeviceIdType.MESH


def dot(a, b):
    return jnp.dot(a, b, preferred_element_type=F32)


def kernel(
    sizes,
    tok_hbm,
    wg_hbm,
    wu_hbm,
    wd_hbm,
    gain_ref,
    ids_ref,
    wt_ref,
    row_ref,
    pi_ref,
    pit_ref,
    out_ref,
    pm_ref,
    pe_ref,
    cm_ref,
    ce_ref,
    post,
    pos_tok,
    w1,
    w2,
    x_buf,
    xs,
    acc,
    part_out,
    part_in,
    first_msg,
    next_msg,
    back_out,
    back_in,
    h_buf,
    w_sem,
    tok_sem,
    a1_send,
    a1_recv,
    a2_send,
    a2_recv,
    b1_send,
    b1_recv,
    b2_send,
    b2_recv,
    h_send,
    h_recv,
    post_send,
    post_recv,
):
    stages, ranks, experts, micro, group = sizes
    sets = experts // group
    chunks = micro * sets
    width = h_buf.shape[2]
    narrow = width // BLOCKS
    hidden = w2.shape[1]
    main_rows = group * ROWS
    extra_rows = xs.shape[1] - main_rows
    model = width * ranks
    tok = h_buf.shape[1]
    p = lax.axis_index("pipe")
    t = lax.axis_index("tensor")
    me = lax.axis_index("expert")
    my_set = lax.rem(me, sets)
    my_place = me // sets

    def peer(i):
        return lax.rem(t + i, ranks)

    def other(i):
        return lax.rem(me + i, experts)

    order = sorted(range(experts), key=lambda i: -min(i // 2, (experts - 1 - i) // 2 + 1 if i > 1 else 0))

    def other_chip(i):
        return lax.rem(me - lax.rem(me, 2) + i, experts)

    def remote(src, dst, send, recv, where):
        return pltpu.make_async_remote_copy(
            src_ref=src, dst_ref=dst, send_sem=send, recv_sem=recv, device_id=where, device_id_type=MESH
        )

    loads = []
    for f in range(ranks):
        rows = pl.ds(f * width, width)
        loads.append(pltpu.make_async_copy(wg_hbm.at[rows, :], w1.at[f, :, pl.ds(0, hidden)], w_sem.at[f]))
        loads.append(pltpu.make_async_copy(wu_hbm.at[rows, :], w1.at[f, :, pl.ds(hidden, hidden)], w_sem.at[ranks + f]))
        loads.append(pltpu.make_async_copy(wd_hbm.at[:, rows], w2.at[f], w_sem.at[2 * ranks + f]))
    slice_start = pl.multiple_of(t * width, 128)
    tok_load = pltpu.make_async_copy(tok_hbm.at[:, :, pl.ds(slice_start, width)], h_buf, tok_sem)

    @pl.when(p == 0)
    def _():
        tok_load.start()

    for load in loads:
        load.start()

    def count(shape, dim):
        return lax.broadcasted_iota(jnp.int32, shape, dim)

    def column(row):
        mine = count((tok, tok), 0) == count((tok, tok), 1)
        return jnp.sum(jnp.where(mine, row.astype(F32), 0.0), axis=1, keepdims=True)

    def slots(m):
        across, down = count((tok, tok), 1), count((tok, tok), 0)
        rank_row = jnp.sum(jnp.where(column(row_ref[m]) == across.astype(F32), down.astype(F32), 0.0), axis=0, keepdims=True)
        rank_col = jnp.sum(jnp.where(row_ref[m] == down, across.astype(F32), 0.0), axis=1, keepdims=True)
        part_row = jnp.floor(rank_row * (ranks / tok))
        part_col = jnp.floor(rank_col * (ranks / tok))
        same = jnp.where(part_row == part_col, 1.0, 0.0)
        before_t = (jnp.where(rank_col < rank_row, 1.0, 0.0) * same).astype(BF16)
        before = (jnp.where(rank_row < rank_col, 1.0, 0.0) * same).astype(BF16)
        e_down, e_across = count((experts, tok), 0), count((tok, experts), 1)
        ids = ids_ref[m]
        named_t = jnp.where((ids[0:1] == e_down) | (ids[1:2] == e_down), 1.0, 0.0)
        first, second = column(ids[0:1]), column(ids[1:2])
        e_across = e_across.astype(F32)
        named = jnp.where((first == e_across) | (second == e_across), 1.0, 0.0)
        slot_t = dot(named_t.astype(BF16), before_t)
        slot = dot(before, named.astype(BF16))
        post[0, m] = jnp.where((named_t > 0.0) & (slot_t < CAP), part_row * CAP + slot_t, -1.0)
        pos_tok[m] = jnp.where((named > 0.0) & (slot < CAP), part_col * CAP + slot, -1.0)

    def place(which, m):
        pos = post[which, m]
        four = jnp.concatenate([pos] * BLOCKS, axis=1)
        plain = count((ROWS, tok), 0).astype(F32)
        down, across = count((ROWS, BLOCKS * tok), 0), count((ROWS, BLOCKS * tok), 1)
        shift = tok.bit_length() - 1
        own = lax.shift_right_logical(across, shift) == lax.shift_right_logical(down, 2)
        slot = jnp.where(own, (ROWS + (down & 3)).astype(F32), -2.0)
        for e in range(experts):
            rows = pl.ds(e * ROWS, ROWS)
            pm_ref[which, m, rows, :] = jnp.where(pos[e : e + 1] == plain, 1.0, 0.0).astype(BF16)
            pe_ref[which, m, rows, :] = jnp.where(four[e : e + 1] == slot, 1.0, 0.0).astype(BF16)

    def gather(m):
        lanes = experts * ROWS
        e_across = count((tok, experts), 1).astype(F32)
        ids, wt = ids_ref[m], wt_ref[m]
        weight = jnp.where(column(ids[0:1]) == e_across, column(wt[0:1]), 0.0)
        weight = weight + jnp.where(column(ids[1:2]) == e_across, column(wt[1:2]), 0.0)
        high = weight.astype(BF16)
        low = (weight - high.astype(F32)).astype(BF16)
        block = lax.shift_right_logical(count((experts, lanes), 1), 4) == count((experts, lanes), 0)
        widen = jnp.where(block, 1.0, 0.0).astype(BF16)
        pos = dot(pos_tok[m].astype(BF16), widen)
        lane = count((tok, lanes), 1)
        inside = lane & (ROWS - 1)
        plain = inside.astype(F32)
        tail = (ROWS + (lane & 3)).astype(F32)
        for n, half in enumerate((high, low)):
            value = dot(half, widen)
            cm_ref[m, pl.ds(n * tok, tok), :] = jnp.where(pos == plain, value, 0.0).astype(BF16)
            for b in range(BLOCKS):
                mine = (pos == tail) & (lax.shift_right_logical(inside, 2) == b)
                ce_ref[m, pl.ds((n * BLOCKS + b) * tok, tok), :] = jnp.where(mine, value, 0.0).astype(BF16)

    for m in range(micro):
        slots(m)

    barrier = pltpu.get_barrier_semaphore()
    for i in range(1, ranks):
        pl.semaphore_signal(barrier, inc=1, device_id={"tensor": peer(i)}, device_id_type=MESH)
    for i in range(1, experts):
        pl.semaphore_signal(barrier, inc=1, device_id={"expert": other(i)}, device_id_type=MESH)

    @pl.when(p < stages - 1)
    def _():
        for e in range(experts):
            pl.semaphore_signal(barrier, inc=1, device_id={"pipe": p + 1, "expert": e}, device_id_type=MESH)

    @pl.when(p > 0)
    def _():
        for e in range(experts):
            pl.semaphore_signal(barrier, inc=1, device_id={"pipe": p - 1, "expert": e}, device_id_type=MESH)

    ahead = jnp.where(p < stages - 1, experts, 0)
    behind = jnp.where(p > 0, experts, 0)
    pl.semaphore_wait(barrier, ranks - 1 + experts - 1 + ahead + behind)

    def fill_messages(msg, which, m, stream):
        main = dot(pm_ref[which, m], stream).astype(BF16)
        stacked = jnp.concatenate([stream[:, b * narrow : (b + 1) * narrow] for b in range(BLOCKS)], axis=0)
        extra = dot(pe_ref[which, m], stacked).astype(BF16)
        for e in range(experts):
            msg[m, e, :, pl.ds(0, width)] = main[e * ROWS : (e + 1) * ROWS]
            msg[m, e, :, pl.ds(width, narrow)] = extra[e * ROWS : (e + 1) * ROWS]

    def first_copy(m, i):
        e = other(i)
        c = m * sets + my_set
        return remote(
            first_msg.at[m, e],
            x_buf.at[c, t, my_place],
            a1_send.at[0, m, e],
            a1_recv.at[c, my_place],
            {"expert": e},
        )

    def next_copy(m, e):
        c = m * sets + my_set
        return remote(
            next_msg.at[m, e],
            x_buf.at[c, t, my_place],
            a1_send.at[1, m, e],
            a1_recv.at[c, my_place],
            {"pipe": p + 1, "expert": e},
        )

    def post_copy():
        return remote(post.at[0], post.at[1], post_send, post_recv, {"pipe": p - 1})

    def stream_copy(m):
        return remote(out_ref.at[m], h_buf.at[m], h_send.at[m], h_recv.at[m], {"pipe": p + 1})

    def relay_copy(c, j, i):
        return remote(
            x_buf.at[c, t, j], x_buf.at[c, t, j], a2_send.at[c, j, i - 1], a2_recv.at[c, t, j], {"tensor": peer(i)}
        )

    def part_copy(c, i):
        return remote(
            part_out.at[c, i - 1], part_in.at[c, t], b1_send.at[c, i - 1], b1_recv.at[c, t], {"tensor": peer(i)}
        )

    def back_copy(c, j):
        m = c // sets
        g = j * sets + lax.rem(c, sets)
        return remote(back_out.at[c, j], back_in.at[m, me], b2_send.at[c, j], b2_recv.at[m, me], {"expert": g})

    def relay(c):
        near = lax.rem((me + experts - lax.rem(c, sets)) // 2, experts // 2) * 2 // sets
        for n in range(group):
            j = lax.rem(near + n, group)
            g = j * sets + lax.rem(c, sets)

            @pl.when((p > 0) | (g != me))
            def _():
                remote(
                    first_msg.at[0, 0], x_buf.at[c, t, j], a1_send.at[0, 0, 0], a1_recv.at[c, j], {"expert": other(1)}
                ).wait_recv()

            for i in (2, 1, 3):
                relay_copy(c, j, i).start()

    def experts_work(c):
        total = None
        squares = None
        for i in (0, 1, 3, 2):
            f = peer(i)
            if i > 0:
                for j in range(group):
                    remote(
                        x_buf.at[c, f, j], x_buf.at[c, f, j], a2_send.at[c, j, i - 1], a2_recv.at[c, f, j], {"tensor": f}
                    ).wait_recv()
            gain = gain_ref[f]
            main = x_buf[c, f, :, :, pl.ds(0, width)].reshape(main_rows, width).astype(F32)
            xs[f, pl.ds(0, main_rows), :] = (main * gain).astype(BF16)
            packed = x_buf[c, f, :, :, pl.ds(width, narrow)].reshape(main_rows, narrow)
            extra = dot(pi_ref[...], packed)
            extra_sq = jnp.zeros((extra_rows, 1), F32)
            for b in range(BLOCKS):
                block = extra[b * extra_rows : (b + 1) * extra_rows]
                cols = slice(b * narrow, (b + 1) * narrow)
                extra_sq = extra_sq + jnp.sum(block * block, axis=1, keepdims=True)
                xs[f, pl.ds(main_rows, extra_rows), pl.ds(b * narrow, narrow)] = (block * gain[:, cols]).astype(BF16)
            sq = jnp.concatenate([jnp.sum(main * main, axis=1, keepdims=True), extra_sq], axis=0)
            squares = sq if squares is None else squares + sq
            if i == 0:
                acc[...] = dot(xs[f], w1[f])
            else:
                acc[...] += dot(xs[f], w1[f])
        inv = lax.rsqrt(squares * (1.0 / model) + EPS)
        gate = acc[:, pl.ds(0, hidden)] * inv
        up = acc[:, pl.ds(hidden, hidden)] * inv
        act = (gate / (1.0 + jnp.exp(-gate)) * up).astype(BF16)
        for i in (2, 1, 3, 0):
            part = dot(act, w2[peer(i)]).astype(BF16)
            extra = part[main_rows:]
            stacked = jnp.concatenate([extra[:, b * narrow : (b + 1) * narrow] for b in range(BLOCKS)], axis=0)
            packed = dot(pit_ref[...], stacked).astype(BF16)
            wide = jnp.concatenate([part[:main_rows], packed], axis=1).reshape(group, ROWS, width + narrow)
            if i == 0:
                part_in[c, t] = wide
            else:
                part_out[c, i - 1] = wide
                part_copy(c, i).start()

    def give_back(c):
        m = c // sets
        for i in range(1, ranks):
            f = peer(i)
            remote(part_out.at[c, i - 1], part_in.at[c, f], b1_send.at[c, i - 1], b1_recv.at[c, f], {"tensor": f}).wait_recv()
        total = part_in[c, 0].astype(F32)
        for q in range(1, ranks):
            total = total + part_in[c, q].astype(F32)
        back_out[c] = total.astype(BF16)
        for j in range(group):
            g = j * sets + lax.rem(c, sets)

            @pl.when(g != me)
            def _():
                back_copy(c, j).start()

            @pl.when(g == me)
            def _():
                back_in[m, me] = back_out[c, j]

    def combine(c):
        m = c // sets

        @pl.when(lax.rem(c, sets) == my_set)
        def _():
            for i in range(1, experts):
                e = other(i)
                remote(back_out.at[c, 0], back_in.at[m, e], b2_send.at[c, 0], b2_recv.at[m, e], {"expert": e}).wait_recv()

            @pl.when(p > 0)
            def _():
                remote(out_ref.at[m], h_buf.at[m], h_send.at[m], h_recv.at[m], {"expert": other(1)}).wait_recv()

            main = back_in[m, :, :, pl.ds(0, width)].reshape(experts * ROWS, width)
            packed = back_in[m, :, :, pl.ds(width, narrow)].reshape(experts * ROWS, narrow)
            wide = dot(cm_ref[m], main)
            update = wide[:tok] + wide[tok:]
            thin = dot(ce_ref[m], packed)
            thin = thin[: BLOCKS * tok] + thin[BLOCKS * tok :]
            spread = jnp.concatenate([thin[b * tok : (b + 1) * tok] for b in range(BLOCKS)], axis=1)
            fresh = (h_buf[m].astype(F32) + update + spread).astype(BF16)
            out_ref[m] = fresh

            @pl.when(p < stages - 1)
            def _():
                fill_messages(next_msg, 1, m, fresh)
                for i in order:
                    next_copy(m, other_chip(i)).start()
                stream_copy(m).start()

    @pl.when(p > 0)
    def _():
        post_copy().start()

    @pl.when(p == 0)
    def _():
        tok_load.wait()
        for m in range(micro):
            place(0, m)
            fill_messages(first_msg, 0, m, h_buf[m])
            for i in range(1, experts):
                first_copy(m, i).start()
            x_buf[m * sets + my_set, t, my_place] = first_msg[m, me]
        relay(0)

    for m in range(micro):
        gather(m)

    @pl.when(p < stages - 1)
    def _():
        remote(post.at[0], post.at[1], post_send, post_recv, {"expert": other(1)}).wait_recv()
        for m in range(micro):
            place(1, m)

    for load in loads:
        load.wait()

    def step(s, carry):
        @pl.when((s < chunks) & ((s > 0) | (p > 0)))
        def _():
            relay(s)

        @pl.when(s > 0)
        def _():
            give_back(s - 1)

        @pl.when(s < chunks)
        def _():
            experts_work(s)

        @pl.when(s > 0)
        def _():
            combine(s - 1)

        return carry

    lax.fori_loop(0, chunks + 1, step, 0)

    @pl.when(p > 0)
    def _():
        post_copy().wait_send()

    @pl.when(p == 0)
    def _():
        for m in range(micro):
            for i in range(1, experts):
                first_copy(m, i).wait_send()

    @pl.when(p < stages - 1)
    def _():
        for m in range(micro):
            for e in range(experts):
                next_copy(m, e).wait_send()
            stream_copy(m).wait_send()

    def drain(c, carry):
        for j in range(group):
            for i in range(1, ranks):
                relay_copy(c, j, i).wait_send()
            g = j * sets + lax.rem(c, sets)

            @pl.when(g != me)
            def _():
                back_copy(c, j).wait_send()

        for i in range(1, ranks):
            part_copy(c, i).wait_send()
        return carry

    lax.fori_loop(0, chunks, drain, 0)


def local(sizes, tokens, gains, route_ids, route_weights, picks, w_gate, w_up, w_down):
    stages, ranks, experts, micro, group = sizes
    tok, model = tokens.shape[1:]
    width = model // ranks
    narrow = width // BLOCKS
    wide = width + narrow
    hidden = w_gate.shape[3]
    chunks = micro * (experts // group)
    main_rows = group * ROWS
    extra_rows = max(ROWS, BLOCKS * group)
    rows = main_rows + extra_rows

    permute = np.zeros((BLOCKS, extra_rows, group, BLOCKS, BLOCKS), np.float32)
    for b in range(BLOCKS):
        for j in range(group):
            for k in range(BLOCKS):
                permute[b, j * BLOCKS + k, j, b, k] = 1.0
    permute = permute.reshape(BLOCKS * extra_rows, main_rows)
    pi = jnp.asarray(permute, BF16)
    pit = jnp.asarray(permute.T.copy(), BF16)

    vmem = pl.BlockSpec(memory_space=pltpu.VMEM)
    hbm = pl.BlockSpec(memory_space=pl.ANY)
    dma = pltpu.SemaphoreType.DMA
    out = pl.pallas_call(
        functools.partial(kernel, sizes),
        out_shape=jax.ShapeDtypeStruct((micro, tok, width), BF16),
        in_specs=[hbm] * 4 + [vmem] * 6,
        out_specs=vmem,
        scratch_shapes=[
            pltpu.VMEM((2, micro, experts * ROWS, tok), BF16),
            pltpu.VMEM((2, micro, experts * ROWS, BLOCKS * tok), BF16),
            pltpu.VMEM((micro, 2 * tok, experts * ROWS), BF16),
            pltpu.VMEM((micro, 2 * BLOCKS * tok, experts * ROWS), BF16),
            pltpu.VMEM((2, micro, experts, tok), F32),
            pltpu.VMEM((micro, tok, experts), F32),
            pltpu.VMEM((ranks, width, 2 * hidden), BF16),
            pltpu.VMEM((ranks, hidden, width), BF16),
            pltpu.VMEM((chunks, ranks, group, ROWS, wide), BF16),
            pltpu.VMEM((ranks, rows, width), BF16),
            pltpu.VMEM((rows, 2 * hidden), F32),
            pltpu.VMEM((chunks, ranks - 1, group, ROWS, wide), BF16),
            pltpu.VMEM((chunks, ranks, group, ROWS, wide), BF16),
            pltpu.VMEM((micro, experts, ROWS, wide), BF16),
            pltpu.VMEM((micro, experts, ROWS, wide), BF16),
            pltpu.VMEM((chunks, group, ROWS, wide), BF16),
            pltpu.VMEM((micro, experts, ROWS, wide), BF16),
            pltpu.VMEM((micro, tok, width), BF16),
            dma((3 * ranks,)),
            dma,
            dma((2, micro, experts)),
            dma((chunks, group)),
            dma((chunks, group, ranks - 1)),
            dma((chunks, ranks, group)),
            dma((chunks, ranks - 1)),
            dma((chunks, ranks)),
            dma((chunks, group)),
            dma((micro, experts)),
            dma((micro,)),
            dma((micro,)),
            dma,
            dma,
        ],
        compiler_params=pltpu.CompilerParams(
            collective_id=0, has_side_effects=True, vmem_limit_bytes=60_000_000
        ),
    )(
        tokens,
        w_gate[0, 0],
        w_up[0, 0],
        w_down[0, 0],
        gains.reshape(ranks, 1, width),
        jnp.swapaxes(route_ids[0], 1, 2),
        jnp.swapaxes(route_weights[0], 1, 2),
        picks[0],
        pi,
        pit,
    )
    return out[None]


def solution(mesh, group=2):
    experts = mesh.shape["expert"]
    sizes = (mesh.shape["pipe"], mesh.shape["tensor"], experts, 2, min(group, experts))
    return jax.shard_map(
        functools.partial(local, sizes),
        mesh=mesh,
        in_specs=(
            P(None, "expert", None),
            P("pipe", None),
            P("pipe", None, "expert", None),
            P("pipe", None, "expert", None),
            P("pipe", None, "expert", None),
            P("pipe", "expert", None, "tensor"),
            P("pipe", "expert", None, "tensor"),
            P("pipe", "expert", "tensor", None),
        ),
        out_specs=P("pipe", None, "expert", "tensor"),
        check_vma=False,
    )
```

```python
import functools

import jax
import jax.numpy as jnp
import numpy as np
from jax import lax
from jax.experimental import pallas as pl
from jax.experimental.pallas import tpu as pltpu
from jax.sharding import PartitionSpec as P

EPS = 1e-06
CAP = 5
ROWS = 16
BLOCKS = 4
F32 = jnp.float32
BF16 = jnp.bfloat16
MESH = pl.DeviceIdType.MESH


def dot(a, b):
    return jnp.dot(a, b, preferred_element_type=F32)


def kernel(
    sizes,
    tok_hbm,
    wg_hbm,
    wu_hbm,
    wd_hbm,
    gain_ref,
    ids_ref,
    wt_ref,
    row_ref,
    pi_ref,
    pit_ref,
    out_ref,
    pm_ref,
    pe_ref,
    cm_ref,
    ce_ref,
    post,
    pos_tok,
    w1,
    w2,
    x_buf,
    xs,
    acc,
    part_out,
    part_in,
    first_msg,
    next_msg,
    back_out,
    back_in,
    h_buf,
    w_sem,
    tok_sem,
    a1_send,
    a1_recv,
    a2_send,
    a2_recv,
    b1_send,
    b1_recv,
    b2_send,
    b2_recv,
    h_send,
    h_recv,
    post_send,
    post_recv,
):
    stages, ranks, experts, micro, group = sizes
    sets = experts // group
    chunks = micro * sets
    width = h_buf.shape[2]
    narrow = width // BLOCKS
    hidden = w2.shape[1]
    main_rows = group * ROWS
    extra_rows = xs.shape[1] - main_rows
    model = width * ranks
    tok = h_buf.shape[1]
    p = lax.axis_index("pipe")
    t = lax.axis_index("tensor")
    me = lax.axis_index("expert")
    my_set = lax.rem(me, sets)
    my_place = me // sets

    def peer(i):
        return lax.rem(t + i, ranks)

    def other(i):
        return lax.rem(me + i, experts)

    order = sorted(range(experts), key=lambda i: -min(i // 2, (experts - 1 - i) // 2 + 1 if i > 1 else 0))

    def other_chip(i):
        return lax.rem(me - lax.rem(me, 2) + i, experts)

    def remote(src, dst, send, recv, where):
        return pltpu.make_async_remote_copy(
            src_ref=src, dst_ref=dst, send_sem=send, recv_sem=recv, device_id=where, device_id_type=MESH
        )

    loads = []
    for f in range(ranks):
        rows = pl.ds(f * width, width)
        loads.append(pltpu.make_async_copy(wg_hbm.at[rows, :], w1.at[f, :, pl.ds(0, hidden)], w_sem.at[f]))
        loads.append(pltpu.make_async_copy(wu_hbm.at[rows, :], w1.at[f, :, pl.ds(hidden, hidden)], w_sem.at[ranks + f]))
        loads.append(pltpu.make_async_copy(wd_hbm.at[:, rows], w2.at[f], w_sem.at[2 * ranks + f]))
    slice_start = pl.multiple_of(t * width, 128)
    tok_load = pltpu.make_async_copy(tok_hbm.at[:, :, pl.ds(slice_start, width)], h_buf, tok_sem)

    @pl.when(p == 0)
    def _():
        tok_load.start()

    for load in loads:
        load.start()

    def count(shape, dim):
        return lax.broadcasted_iota(jnp.int32, shape, dim)

    def column(row):
        mine = count((tok, tok), 0) == count((tok, tok), 1)
        return jnp.sum(jnp.where(mine, row.astype(F32), 0.0), axis=1, keepdims=True)

    def slots(m):
        across, down = count((tok, tok), 1), count((tok, tok), 0)
        rank_row = jnp.sum(jnp.where(column(row_ref[m]) == across.astype(F32), down.astype(F32), 0.0), axis=0, keepdims=True)
        rank_col = jnp.sum(jnp.where(row_ref[m] == down, across.astype(F32), 0.0), axis=1, keepdims=True)
        part_row = jnp.floor(rank_row * (ranks / tok))
        part_col = jnp.floor(rank_col * (ranks / tok))
        same = jnp.where(part_row == part_col, 1.0, 0.0)
        before_t = (jnp.where(rank_col < rank_row, 1.0, 0.0) * same).astype(BF16)
        before = (jnp.where(rank_row < rank_col, 1.0, 0.0) * same).astype(BF16)
        e_down, e_across = count((experts, tok), 0), count((tok, experts), 1)
        ids = ids_ref[m]
        named_t = jnp.where((ids[0:1] == e_down) | (ids[1:2] == e_down), 1.0, 0.0)
        first, second = column(ids[0:1]), column(ids[1:2])
        e_across = e_across.astype(F32)
        named = jnp.where((first == e_across) | (second == e_across), 1.0, 0.0)
        slot_t = dot(named_t.astype(BF16), before_t)
        slot = dot(before, named.astype(BF16))
        post[0, m] = jnp.where((named_t > 0.0) & (slot_t < CAP), part_row * CAP + slot_t, -1.0)
        pos_tok[m] = jnp.where((named > 0.0) & (slot < CAP), part_col * CAP + slot, -1.0)

    def place(which, m):
        pos = post[which, m]
        four = jnp.concatenate([pos] * BLOCKS, axis=1)
        plain = count((ROWS, tok), 0).astype(F32)
        down, across = count((ROWS, BLOCKS * tok), 0), count((ROWS, BLOCKS * tok), 1)
        shift = tok.bit_length() - 1
        own = lax.shift_right_logical(across, shift) == lax.shift_right_logical(down, 2)
        slot = jnp.where(own, (ROWS + (down & 3)).astype(F32), -2.0)
        for e in range(experts):
            rows = pl.ds(e * ROWS, ROWS)
            pm_ref[which, m, rows, :] = jnp.where(pos[e : e + 1] == plain, 1.0, 0.0).astype(BF16)
            pe_ref[which, m, rows, :] = jnp.where(four[e : e + 1] == slot, 1.0, 0.0).astype(BF16)

    def gather(m):
        lanes = experts * ROWS
        e_across = count((tok, experts), 1).astype(F32)
        ids, wt = ids_ref[m], wt_ref[m]
        weight = jnp.where(column(ids[0:1]) == e_across, column(wt[0:1]), 0.0)
        weight = weight + jnp.where(column(ids[1:2]) == e_across, column(wt[1:2]), 0.0)
        high = weight.astype(BF16)
        low = (weight - high.astype(F32)).astype(BF16)
        block = lax.shift_right_logical(count((experts, lanes), 1), 4) == count((experts, lanes), 0)
        widen = jnp.where(block, 1.0, 0.0).astype(BF16)
        pos = dot(pos_tok[m].astype(BF16), widen)
        lane = count((tok, lanes), 1)
        inside = lane & (ROWS - 1)
        plain = inside.astype(F32)
        tail = (ROWS + (lane & 3)).astype(F32)
        for n, half in enumerate((high, low)):
            value = dot(half, widen)
            cm_ref[m, pl.ds(n * tok, tok), :] = jnp.where(pos == plain, value, 0.0).astype(BF16)
            for b in range(BLOCKS):
                mine = (pos == tail) & (lax.shift_right_logical(inside, 2) == b)
                ce_ref[m, pl.ds((n * BLOCKS + b) * tok, tok), :] = jnp.where(mine, value, 0.0).astype(BF16)

    for m in range(micro):
        slots(m)

    barrier = pltpu.get_barrier_semaphore()
    for i in range(1, ranks):
        pl.semaphore_signal(barrier, inc=1, device_id={"tensor": peer(i)}, device_id_type=MESH)
    for i in range(1, experts):
        pl.semaphore_signal(barrier, inc=1, device_id={"expert": other(i)}, device_id_type=MESH)

    @pl.when(p < stages - 1)
    def _():
        for e in range(experts):
            pl.semaphore_signal(barrier, inc=1, device_id={"pipe": p + 1, "expert": e}, device_id_type=MESH)

    @pl.when(p > 0)
    def _():
        for e in range(experts):
            pl.semaphore_signal(barrier, inc=1, device_id={"pipe": p - 1, "expert": e}, device_id_type=MESH)

    ahead = jnp.where(p < stages - 1, experts, 0)
    behind = jnp.where(p > 0, experts, 0)
    pl.semaphore_wait(barrier, ranks - 1 + experts - 1 + ahead + behind)

    def fill_messages(msg, which, m, stream):
        main = dot(pm_ref[which, m], stream).astype(BF16)
        stacked = jnp.concatenate([stream[:, b * narrow : (b + 1) * narrow] for b in range(BLOCKS)], axis=0)
        extra = dot(pe_ref[which, m], stacked).astype(BF16)
        for e in range(experts):
            msg[m, e, :, pl.ds(0, width)] = main[e * ROWS : (e + 1) * ROWS]
            msg[m, e, :, pl.ds(width, narrow)] = extra[e * ROWS : (e + 1) * ROWS]

    def first_copy(m, i):
        e = other(i)
        c = m * sets + my_set
        return remote(
            first_msg.at[m, e],
            x_buf.at[c, t, my_place],
            a1_send.at[0, m, e],
            a1_recv.at[c, my_place],
            {"expert": e},
        )

    def next_copy(m, e):
        c = m * sets + my_set
        return remote(
            next_msg.at[m, e],
            x_buf.at[c, t, my_place],
            a1_send.at[1, m, e],
            a1_recv.at[c, my_place],
            {"pipe": p + 1, "expert": e},
        )

    def post_copy():
        return remote(post.at[0], post.at[1], post_send, post_recv, {"pipe": p - 1})

    def stream_copy(m):
        return remote(out_ref.at[m], h_buf.at[m], h_send.at[m], h_recv.at[m], {"pipe": p + 1})

    def relay_copy(c, j, i):
        return remote(
            x_buf.at[c, t, j], x_buf.at[c, t, j], a2_send.at[c, j, i - 1], a2_recv.at[c, t, j], {"tensor": peer(i)}
        )

    def part_copy(c, i):
        return remote(
            part_out.at[c, i - 1], part_in.at[c, t], b1_send.at[c, i - 1], b1_recv.at[c, t], {"tensor": peer(i)}
        )

    def back_copy(c, j):
        m = c // sets
        g = j * sets + lax.rem(c, sets)
        return remote(back_out.at[c, j], back_in.at[m, me], b2_send.at[c, j], b2_recv.at[m, me], {"expert": g})

    def relay(c):
        near = lax.rem((me + experts - lax.rem(c, sets)) // 2, experts // 2) * 2 // sets
        for n in range(group):
            j = lax.rem(near + n, group)
            g = j * sets + lax.rem(c, sets)

            @pl.when((p > 0) | (g != me))
            def _():
                remote(
                    first_msg.at[0, 0], x_buf.at[c, t, j], a1_send.at[0, 0, 0], a1_recv.at[c, j], {"expert": other(1)}
                ).wait_recv()

            for i in (2, 1, 3):
                relay_copy(c, j, i).start()

    def experts_work(c):
        total = None
        squares = None
        for i in (0, 1, 3, 2):
            f = peer(i)
            if i > 0:
                for j in range(group):
                    remote(
                        x_buf.at[c, f, j], x_buf.at[c, f, j], a2_send.at[c, j, i - 1], a2_recv.at[c, f, j], {"tensor": f}
                    ).wait_recv()
            gain = gain_ref[f]
            main = x_buf[c, f, :, :, pl.ds(0, width)].reshape(main_rows, width).astype(F32)
            xs[f, pl.ds(0, main_rows), :] = (main * gain).astype(BF16)
            packed = x_buf[c, f, :, :, pl.ds(width, narrow)].reshape(main_rows, narrow)
            extra = dot(pi_ref[...], packed)
            extra_sq = jnp.zeros((extra_rows, 1), F32)
            for b in range(BLOCKS):
                block = extra[b * extra_rows : (b + 1) * extra_rows]
                cols = slice(b * narrow, (b + 1) * narrow)
                extra_sq = extra_sq + jnp.sum(block * block, axis=1, keepdims=True)
                xs[f, pl.ds(main_rows, extra_rows), pl.ds(b * narrow, narrow)] = (block * gain[:, cols]).astype(BF16)
            sq = jnp.concatenate([jnp.sum(main * main, axis=1, keepdims=True), extra_sq], axis=0)
            squares = sq if squares is None else squares + sq
            if i == 0:
                acc[...] = dot(xs[f], w1[f])
            else:
                acc[...] += dot(xs[f], w1[f])
        inv = lax.rsqrt(squares * (1.0 / model) + EPS)
        gate = acc[:, pl.ds(0, hidden)] * inv
        up = acc[:, pl.ds(hidden, hidden)] * inv
        act = (gate / (1.0 + jnp.exp(-gate)) * up).astype(BF16)
        for i in (2, 1, 3, 0):
            part = dot(act, w2[peer(i)]).astype(BF16)
            extra = part[main_rows:]
            stacked = jnp.concatenate([extra[:, b * narrow : (b + 1) * narrow] for b in range(BLOCKS)], axis=0)
            packed = dot(pit_ref[...], stacked).astype(BF16)
            wide = jnp.concatenate([part[:main_rows], packed], axis=1).reshape(group, ROWS, width + narrow)
            if i == 0:
                part_in[c, t] = wide
            else:
                part_out[c, i - 1] = wide
                part_copy(c, i).start()

    def give_back(c):
        m = c // sets
        for i in range(1, ranks):
            f = peer(i)
            remote(part_out.at[c, i - 1], part_in.at[c, f], b1_send.at[c, i - 1], b1_recv.at[c, f], {"tensor": f}).wait_recv()
        total = part_in[c, 0].astype(F32)
        for q in range(1, ranks):
            total = total + part_in[c, q].astype(F32)
        back_out[c] = total.astype(BF16)
        for j in range(group):
            g = j * sets + lax.rem(c, sets)

            @pl.when(g != me)
            def _():
                back_copy(c, j).start()

            @pl.when(g == me)
            def _():
                back_in[m, me] = back_out[c, j]

    def combine(c):
        m = c // sets

        @pl.when(lax.rem(c, sets) == my_set)
        def _():
            for i in range(1, experts):
                e = other(i)
                remote(back_out.at[c, 0], back_in.at[m, e], b2_send.at[c, 0], b2_recv.at[m, e], {"expert": e}).wait_recv()

            @pl.when(p > 0)
            def _():
                remote(out_ref.at[m], h_buf.at[m], h_send.at[m], h_recv.at[m], {"expert": other(1)}).wait_recv()

            main = back_in[m, :, :, pl.ds(0, width)].reshape(experts * ROWS, width)
            packed = back_in[m, :, :, pl.ds(width, narrow)].reshape(experts * ROWS, narrow)
            wide = dot(cm_ref[m], main)
            update = wide[:tok] + wide[tok:]
            thin = dot(ce_ref[m], packed)
            thin = thin[: BLOCKS * tok] + thin[BLOCKS * tok :]
            spread = jnp.concatenate([thin[b * tok : (b + 1) * tok] for b in range(BLOCKS)], axis=1)
            fresh = (h_buf[m].astype(F32) + update + spread).astype(BF16)
            out_ref[m] = fresh

            @pl.when(p < stages - 1)
            def _():
                fill_messages(next_msg, 1, m, fresh)
                for i in order:
                    next_copy(m, other_chip(i)).start()
                stream_copy(m).start()

    @pl.when(p > 0)
    def _():
        post_copy().start()

    def start(m):
        fill_messages(first_msg, 0, m, h_buf[m])
        for i in sorted(range(1, experts), key=lambda i: abs(2 * i - experts)):
            first_copy(m, i).start()
        x_buf[m * sets + my_set, t, my_place] = first_msg[m, me]

    @pl.when(p == 0)
    def _():
        tok_load.wait()
        for m in range(micro):
            place(0, m)

        @pl.when(my_set == 0)
        def _():
            start(0)

    for m in range(micro):
        gather(m)

    @pl.when(p < stages - 1)
    def _():
        remote(post.at[0], post.at[1], post_send, post_recv, {"expert": other(1)}).wait_recv()
        for m in range(micro):
            place(1, m)

    @pl.when(p == 0)
    def _():
        @pl.when(my_set > 0)
        def _():
            start(0)

        for m in range(1, micro):
            start(m)

    for load in loads:
        load.wait()

    def step(s, carry):
        @pl.when(s < chunks)
        def _():
            relay(s)

        @pl.when(s > 0)
        def _():
            give_back(s - 1)

        @pl.when(s < chunks)
        def _():
            experts_work(s)

        @pl.when(s > 0)
        def _():
            combine(s - 1)

        return carry

    lax.fori_loop(0, chunks + 1, step, 0)

    @pl.when(p > 0)
    def _():
        post_copy().wait_send()

    @pl.when(p == 0)
    def _():
        for m in range(micro):
            for i in range(1, experts):
                first_copy(m, i).wait_send()

    @pl.when(p < stages - 1)
    def _():
        for m in range(micro):
            for e in range(experts):
                next_copy(m, e).wait_send()
            stream_copy(m).wait_send()

    def drain(c, carry):
        for j in range(group):
            for i in range(1, ranks):
                relay_copy(c, j, i).wait_send()
            g = j * sets + lax.rem(c, sets)

            @pl.when(g != me)
            def _():
                back_copy(c, j).wait_send()

        for i in range(1, ranks):
            part_copy(c, i).wait_send()
        return carry

    lax.fori_loop(0, chunks, drain, 0)


def local(sizes, tokens, gains, route_ids, route_weights, picks, w_gate, w_up, w_down):
    stages, ranks, experts, micro, group = sizes
    tok, model = tokens.shape[1:]
    width = model // ranks
    narrow = width // BLOCKS
    wide = width + narrow
    hidden = w_gate.shape[3]
    chunks = micro * (experts // group)
    main_rows = group * ROWS
    extra_rows = max(ROWS, BLOCKS * group)
    rows = main_rows + extra_rows

    permute = np.zeros((BLOCKS, extra_rows, group, BLOCKS, BLOCKS), np.float32)
    for b in range(BLOCKS):
        for j in range(group):
            for k in range(BLOCKS):
                permute[b, j * BLOCKS + k, j, b, k] = 1.0
    permute = permute.reshape(BLOCKS * extra_rows, main_rows)
    pi = jnp.asarray(permute, BF16)
    pit = jnp.asarray(permute.T.copy(), BF16)

    vmem = pl.BlockSpec(memory_space=pltpu.VMEM)
    hbm = pl.BlockSpec(memory_space=pl.ANY)
    dma = pltpu.SemaphoreType.DMA
    out = pl.pallas_call(
        functools.partial(kernel, sizes),
        out_shape=jax.ShapeDtypeStruct((micro, tok, width), BF16),
        in_specs=[hbm] * 4 + [vmem] * 6,
        out_specs=vmem,
        scratch_shapes=[
            pltpu.VMEM((2, micro, experts * ROWS, tok), BF16),
            pltpu.VMEM((2, micro, experts * ROWS, BLOCKS * tok), BF16),
            pltpu.VMEM((micro, 2 * tok, experts * ROWS), BF16),
            pltpu.VMEM((micro, 2 * BLOCKS * tok, experts * ROWS), BF16),
            pltpu.VMEM((2, micro, experts, tok), F32),
            pltpu.VMEM((micro, tok, experts), F32),
            pltpu.VMEM((ranks, width, 2 * hidden), BF16),
            pltpu.VMEM((ranks, hidden, width), BF16),
            pltpu.VMEM((chunks, ranks, group, ROWS, wide), BF16),
            pltpu.VMEM((ranks, rows, width), BF16),
            pltpu.VMEM((rows, 2 * hidden), F32),
            pltpu.VMEM((chunks, ranks - 1, group, ROWS, wide), BF16),
            pltpu.VMEM((chunks, ranks, group, ROWS, wide), BF16),
            pltpu.VMEM((micro, experts, ROWS, wide), BF16),
            pltpu.VMEM((micro, experts, ROWS, wide), BF16),
            pltpu.VMEM((chunks, group, ROWS, wide), BF16),
            pltpu.VMEM((micro, experts, ROWS, wide), BF16),
            pltpu.VMEM((micro, tok, width), BF16),
            dma((3 * ranks,)),
            dma,
            dma((2, micro, experts)),
            dma((chunks, group)),
            dma((chunks, group, ranks - 1)),
            dma((chunks, ranks, group)),
            dma((chunks, ranks - 1)),
            dma((chunks, ranks)),
            dma((chunks, group)),
            dma((micro, experts)),
            dma((micro,)),
            dma((micro,)),
            dma,
            dma,
        ],
        compiler_params=pltpu.CompilerParams(
            collective_id=0, has_side_effects=True, vmem_limit_bytes=60_000_000
        ),
    )(
        tokens,
        w_gate[0, 0],
        w_up[0, 0],
        w_down[0, 0],
        gains.reshape(ranks, 1, width),
        jnp.swapaxes(route_ids[0], 1, 2),
        jnp.swapaxes(route_weights[0], 1, 2),
        picks[0],
        pi,
        pit,
    )
    return out[None]


def solution(mesh, group=2):
    experts = mesh.shape["expert"]
    sizes = (mesh.shape["pipe"], mesh.shape["tensor"], experts, 2, min(group, experts))
    return jax.shard_map(
        functools.partial(local, sizes),
        mesh=mesh,
        in_specs=(
            P(None, "expert", None),
            P("pipe", None),
            P("pipe", None, "expert", None),
            P("pipe", None, "expert", None),
            P("pipe", None, "expert", None),
            P("pipe", "expert", None, "tensor"),
            P("pipe", "expert", None, "tensor"),
            P("pipe", "expert", "tensor", None),
        ),
        out_specs=P("pipe", None, "expert", "tensor"),
        check_vma=False,
    )
```

```python
import functools

import jax
import jax.numpy as jnp
import numpy as np
from jax import lax
from jax.experimental import pallas as pl
from jax.experimental.pallas import tpu as pltpu
from jax.sharding import PartitionSpec as P

EPS = 1e-06
CAP = 5
ROWS = 16
BLOCKS = 4
F32 = jnp.float32
BF16 = jnp.bfloat16
MESH = pl.DeviceIdType.MESH


def dot(a, b):
    return jnp.dot(a, b, preferred_element_type=F32)


def kernel(
    sizes,
    tok_hbm,
    wg_hbm,
    wu_hbm,
    wd_hbm,
    gain_ref,
    ids_ref,
    wt_ref,
    row_ref,
    pi_ref,
    pit_ref,
    out_ref,
    pm_ref,
    pe_ref,
    cm_ref,
    ce_ref,
    post,
    pos_tok,
    w1,
    w2,
    x_buf,
    xs,
    acc,
    part_out,
    part_in,
    first_msg,
    next_msg,
    back_out,
    back_in,
    h_buf,
    w_sem,
    tok_sem,
    a1_send,
    a1_recv,
    a2_send,
    a2_recv,
    b1_send,
    b1_recv,
    b2_send,
    b2_recv,
    h_send,
    h_recv,
    post_send,
    post_recv,
):
    stages, ranks, experts, micro, group = sizes
    sets = experts // group
    chunks = micro * sets
    width = h_buf.shape[2]
    narrow = width // BLOCKS
    hidden = w2.shape[1]
    main_rows = group * ROWS
    extra_rows = xs.shape[1] - main_rows
    model = width * ranks
    tok = h_buf.shape[1]
    p = lax.axis_index("pipe")
    t = lax.axis_index("tensor")
    me = lax.axis_index("expert")
    my_set = lax.rem(me, sets)
    my_place = me // sets

    def peer(i):
        return lax.rem(t + i, ranks)

    def other(i):
        return lax.rem(me + i, experts)

    order = sorted(range(experts), key=lambda i: -min(i // 2, (experts - 1 - i) // 2 + 1 if i > 1 else 0))

    def other_chip(i):
        return lax.rem(me - lax.rem(me, 2) + i, experts)

    def remote(src, dst, send, recv, where):
        return pltpu.make_async_remote_copy(
            src_ref=src, dst_ref=dst, send_sem=send, recv_sem=recv, device_id=where, device_id_type=MESH
        )

    loads = []
    for f in range(ranks):
        rows = pl.ds(f * width, width)
        loads.append(pltpu.make_async_copy(wg_hbm.at[rows, :], w1.at[f, :, pl.ds(0, hidden)], w_sem.at[f]))
        loads.append(pltpu.make_async_copy(wu_hbm.at[rows, :], w1.at[f, :, pl.ds(hidden, hidden)], w_sem.at[ranks + f]))
        loads.append(pltpu.make_async_copy(wd_hbm.at[:, rows], w2.at[f], w_sem.at[2 * ranks + f]))
    slice_start = pl.multiple_of(t * width, 128)
    tok_load = pltpu.make_async_copy(tok_hbm.at[:, :, pl.ds(slice_start, width)], h_buf, tok_sem)

    @pl.when(p == 0)
    def _():
        tok_load.start()

    for load in loads:
        load.start()

    def count(shape, dim):
        return lax.broadcasted_iota(jnp.int32, shape, dim)

    def column(row):
        mine = count((tok, tok), 0) == count((tok, tok), 1)
        return jnp.sum(jnp.where(mine, row.astype(F32), 0.0), axis=1, keepdims=True)

    def slots(m):
        across, down = count((tok, tok), 1), count((tok, tok), 0)
        rank_row = jnp.sum(jnp.where(column(row_ref[m]) == across.astype(F32), down.astype(F32), 0.0), axis=0, keepdims=True)
        rank_col = jnp.sum(jnp.where(row_ref[m] == down, across.astype(F32), 0.0), axis=1, keepdims=True)
        part_row = jnp.floor(rank_row * (ranks / tok))
        part_col = jnp.floor(rank_col * (ranks / tok))
        same = jnp.where(part_row == part_col, 1.0, 0.0)
        before_t = (jnp.where(rank_col < rank_row, 1.0, 0.0) * same).astype(BF16)
        before = (jnp.where(rank_row < rank_col, 1.0, 0.0) * same).astype(BF16)
        e_down, e_across = count((experts, tok), 0), count((tok, experts), 1)
        ids = ids_ref[m]
        named_t = jnp.where((ids[0:1] == e_down) | (ids[1:2] == e_down), 1.0, 0.0)
        first, second = column(ids[0:1]), column(ids[1:2])
        e_across = e_across.astype(F32)
        named = jnp.where((first == e_across) | (second == e_across), 1.0, 0.0)
        slot_t = dot(named_t.astype(BF16), before_t)
        slot = dot(before, named.astype(BF16))
        post[0, m] = jnp.where((named_t > 0.0) & (slot_t < CAP), part_row * CAP + slot_t, -1.0)
        pos_tok[m] = jnp.where((named > 0.0) & (slot < CAP), part_col * CAP + slot, -1.0)

    def place(which, m):
        pos = post[which, m]
        four = jnp.concatenate([pos] * BLOCKS, axis=1)
        plain = count((ROWS, tok), 0).astype(F32)
        down, across = count((ROWS, BLOCKS * tok), 0), count((ROWS, BLOCKS * tok), 1)
        shift = tok.bit_length() - 1
        own = lax.shift_right_logical(across, shift) == lax.shift_right_logical(down, 2)
        slot = jnp.where(own, (ROWS + (down & 3)).astype(F32), -2.0)
        for e in range(experts):
            rows = pl.ds(e * ROWS, ROWS)
            pm_ref[which, m, rows, :] = jnp.where(pos[e : e + 1] == plain, 1.0, 0.0).astype(BF16)
            pe_ref[which, m, rows, :] = jnp.where(four[e : e + 1] == slot, 1.0, 0.0).astype(BF16)

    def gather(m):
        lanes = experts * ROWS
        e_across = count((tok, experts), 1).astype(F32)
        ids, wt = ids_ref[m], wt_ref[m]
        weight = jnp.where(column(ids[0:1]) == e_across, column(wt[0:1]), 0.0)
        weight = weight + jnp.where(column(ids[1:2]) == e_across, column(wt[1:2]), 0.0)
        high = weight.astype(BF16)
        low = (weight - high.astype(F32)).astype(BF16)
        block = lax.shift_right_logical(count((experts, lanes), 1), 4) == count((experts, lanes), 0)
        widen = jnp.where(block, 1.0, 0.0).astype(BF16)
        pos = dot(pos_tok[m].astype(BF16), widen)
        lane = count((tok, lanes), 1)
        inside = lane & (ROWS - 1)
        plain = inside.astype(F32)
        tail = (ROWS + (lane & 3)).astype(F32)
        for n, half in enumerate((high, low)):
            value = dot(half, widen)
            cm_ref[m, pl.ds(n * tok, tok), :] = jnp.where(pos == plain, value, 0.0).astype(BF16)
            for b in range(BLOCKS):
                mine = (pos == tail) & (lax.shift_right_logical(inside, 2) == b)
                ce_ref[m, pl.ds((n * BLOCKS + b) * tok, tok), :] = jnp.where(mine, value, 0.0).astype(BF16)

    for m in range(micro):
        slots(m)

    barrier = pltpu.get_barrier_semaphore()
    for i in range(1, ranks):
        pl.semaphore_signal(barrier, inc=1, device_id={"tensor": peer(i)}, device_id_type=MESH)
    for i in range(1, experts):
        pl.semaphore_signal(barrier, inc=1, device_id={"expert": other(i)}, device_id_type=MESH)

    @pl.when(p < stages - 1)
    def _():
        for e in range(experts):
            pl.semaphore_signal(barrier, inc=1, device_id={"pipe": p + 1, "expert": e}, device_id_type=MESH)

    @pl.when(p > 0)
    def _():
        for e in range(experts):
            pl.semaphore_signal(barrier, inc=1, device_id={"pipe": p - 1, "expert": e}, device_id_type=MESH)

    ahead = jnp.where(p < stages - 1, experts, 0)
    behind = jnp.where(p > 0, experts, 0)
    pl.semaphore_wait(barrier, ranks - 1 + experts - 1 + ahead + behind)

    def fill_messages(msg, which, m, stream):
        main = dot(pm_ref[which, m], stream).astype(BF16)
        stacked = jnp.concatenate([stream[:, b * narrow : (b + 1) * narrow] for b in range(BLOCKS)], axis=0)
        extra = dot(pe_ref[which, m], stacked).astype(BF16)
        for e in range(experts):
            msg[m, e, :, pl.ds(0, width)] = main[e * ROWS : (e + 1) * ROWS]
            msg[m, e, :, pl.ds(width, narrow)] = extra[e * ROWS : (e + 1) * ROWS]

    def first_copy(m, i):
        e = other(i)
        c = m * sets + my_set
        return remote(
            first_msg.at[m, e],
            x_buf.at[c, t, my_place],
            a1_send.at[0, m, e],
            a1_recv.at[c, my_place],
            {"expert": e},
        )

    def next_copy(m, e):
        c = m * sets + my_set
        return remote(
            next_msg.at[m, e],
            x_buf.at[c, t, my_place],
            a1_send.at[1, m, e],
            a1_recv.at[c, my_place],
            {"pipe": p + 1, "expert": e},
        )

    def post_copy():
        return remote(post.at[0], post.at[1], post_send, post_recv, {"pipe": p - 1})

    def stream_copy(m):
        return remote(out_ref.at[m], h_buf.at[m], h_send.at[m], h_recv.at[m], {"pipe": p + 1})

    def relay_copy(c, j, i):
        return remote(
            x_buf.at[c, t, j], x_buf.at[c, t, j], a2_send.at[c, j, i - 1], a2_recv.at[c, t, j], {"tensor": peer(i)}
        )

    def part_copy(c, i):
        return remote(
            part_out.at[c, i - 1], part_in.at[c, t], b1_send.at[c, i - 1], b1_recv.at[c, t], {"tensor": peer(i)}
        )

    def back_copy(c, j):
        m = c // sets
        g = j * sets + lax.rem(c, sets)
        return remote(back_out.at[c, j], back_in.at[m, me], b2_send.at[c, j], b2_recv.at[m, me], {"expert": g})

    def relay(c):
        near = lax.rem((me + experts - lax.rem(c, sets)) // 2, experts // 2) * 2 // sets
        for n in range(group):
            j = lax.rem(near + n, group)
            g = j * sets + lax.rem(c, sets)

            @pl.when((p > 0) | (g != me))
            def _():
                remote(
                    first_msg.at[0, 0], x_buf.at[c, t, j], a1_send.at[0, 0, 0], a1_recv.at[c, j], {"expert": other(1)}
                ).wait_recv()

            for i in (1, 3, 2):
                relay_copy(c, j, i).start()

    def experts_work(c):
        total = None
        squares = None
        for i in (0, 1, 3, 2):
            f = peer(i)
            if i > 0:
                for j in range(group):
                    remote(
                        x_buf.at[c, f, j], x_buf.at[c, f, j], a2_send.at[c, j, i - 1], a2_recv.at[c, f, j], {"tensor": f}
                    ).wait_recv()
            gain = gain_ref[f]
            main = x_buf[c, f, :, :, pl.ds(0, width)].reshape(main_rows, width).astype(F32)
            xs[f, pl.ds(0, main_rows), :] = (main * gain).astype(BF16)
            packed = x_buf[c, f, :, :, pl.ds(width, narrow)].reshape(main_rows, narrow)
            extra = dot(pi_ref[...], packed)
            extra_sq = jnp.zeros((extra_rows, 1), F32)
            for b in range(BLOCKS):
                block = extra[b * extra_rows : (b + 1) * extra_rows]
                cols = slice(b * narrow, (b + 1) * narrow)
                extra_sq = extra_sq + jnp.sum(block * block, axis=1, keepdims=True)
                xs[f, pl.ds(main_rows, extra_rows), pl.ds(b * narrow, narrow)] = (block * gain[:, cols]).astype(BF16)
            sq = jnp.concatenate([jnp.sum(main * main, axis=1, keepdims=True), extra_sq], axis=0)
            squares = sq if squares is None else squares + sq
            if i == 0:
                acc[...] = dot(xs[f], w1[f])
            else:
                acc[...] += dot(xs[f], w1[f])
        inv = lax.rsqrt(squares * (1.0 / model) + EPS)
        gate = acc[:, pl.ds(0, hidden)] * inv
        up = acc[:, pl.ds(hidden, hidden)] * inv
        act = (gate / (1.0 + jnp.exp(-gate)) * up).astype(BF16)
        for i in (2, 1, 3, 0):
            part = dot(act, w2[peer(i)]).astype(BF16)
            extra = part[main_rows:]
            stacked = jnp.concatenate([extra[:, b * narrow : (b + 1) * narrow] for b in range(BLOCKS)], axis=0)
            packed = dot(pit_ref[...], stacked).astype(BF16)
            wide = jnp.concatenate([part[:main_rows], packed], axis=1).reshape(group, ROWS, width + narrow)
            if i == 0:
                part_in[c, t] = wide
            else:
                part_out[c, i - 1] = wide
                part_copy(c, i).start()

    def give_back(c):
        m = c // sets
        for i in range(1, ranks):
            f = peer(i)
            remote(part_out.at[c, i - 1], part_in.at[c, f], b1_send.at[c, i - 1], b1_recv.at[c, f], {"tensor": f}).wait_recv()
        total = part_in[c, 0].astype(F32)
        for q in range(1, ranks):
            total = total + part_in[c, q].astype(F32)
        back_out[c] = total.astype(BF16)
        for j in range(group):
            g = j * sets + lax.rem(c, sets)

            @pl.when(g != me)
            def _():
                back_copy(c, j).start()

            @pl.when(g == me)
            def _():
                back_in[m, me] = back_out[c, j]

    def combine(c):
        m = c // sets

        @pl.when(lax.rem(c, sets) == my_set)
        def _():
            for i in range(1, experts):
                e = other(i)
                remote(back_out.at[c, 0], back_in.at[m, e], b2_send.at[c, 0], b2_recv.at[m, e], {"expert": e}).wait_recv()

            @pl.when(p > 0)
            def _():
                remote(out_ref.at[m], h_buf.at[m], h_send.at[m], h_recv.at[m], {"expert": other(1)}).wait_recv()

            main = back_in[m, :, :, pl.ds(0, width)].reshape(experts * ROWS, width)
            packed = back_in[m, :, :, pl.ds(width, narrow)].reshape(experts * ROWS, narrow)
            wide = dot(cm_ref[m], main)
            update = wide[:tok] + wide[tok:]
            thin = dot(ce_ref[m], packed)
            thin = thin[: BLOCKS * tok] + thin[BLOCKS * tok :]
            spread = jnp.concatenate([thin[b * tok : (b + 1) * tok] for b in range(BLOCKS)], axis=1)
            fresh = (h_buf[m].astype(F32) + update + spread).astype(BF16)
            out_ref[m] = fresh

            @pl.when(p < stages - 1)
            def _():
                fill_messages(next_msg, 1, m, fresh)
                for i in order:
                    next_copy(m, other_chip(i)).start()
                stream_copy(m).start()

    @pl.when(p > 0)
    def _():
        post_copy().start()

    def start(m):
        fill_messages(first_msg, 0, m, h_buf[m])
        for i in sorted(range(1, experts), key=lambda i: abs(2 * i - experts)):
            first_copy(m, i).start()
        x_buf[m * sets + my_set, t, my_place] = first_msg[m, me]

    @pl.when(p == 0)
    def _():
        tok_load.wait()
        for m in range(micro):
            place(0, m)

        @pl.when(my_set == 0)
        def _():
            start(0)

    for m in range(micro):
        gather(m)

    @pl.when(p < stages - 1)
    def _():
        remote(post.at[0], post.at[1], post_send, post_recv, {"expert": other(1)}).wait_recv()
        for m in range(micro):
            place(1, m)

    @pl.when(p == 0)
    def _():
        @pl.when(my_set > 0)
        def _():
            start(0)

        for m in range(1, micro):
            start(m)

    for load in loads:
        load.wait()

    def step(s, carry):
        @pl.when(s < chunks)
        def _():
            relay(s)

        @pl.when(s > 0)
        def _():
            give_back(s - 1)

        @pl.when(s < chunks)
        def _():
            experts_work(s)

        @pl.when(s > 0)
        def _():
            combine(s - 1)

        return carry

    lax.fori_loop(0, chunks + 1, step, 0)

    @pl.when(p > 0)
    def _():
        post_copy().wait_send()

    @pl.when(p == 0)
    def _():
        for m in range(micro):
            for i in range(1, experts):
                first_copy(m, i).wait_send()

    @pl.when(p < stages - 1)
    def _():
        for m in range(micro):
            for e in range(experts):
                next_copy(m, e).wait_send()
            stream_copy(m).wait_send()

    def drain(c, carry):
        for j in range(group):
            for i in range(1, ranks):
                relay_copy(c, j, i).wait_send()
            g = j * sets + lax.rem(c, sets)

            @pl.when(g != me)
            def _():
                back_copy(c, j).wait_send()

        for i in range(1, ranks):
            part_copy(c, i).wait_send()
        return carry

    lax.fori_loop(0, chunks, drain, 0)


def local(sizes, tokens, gains, route_ids, route_weights, picks, w_gate, w_up, w_down):
    stages, ranks, experts, micro, group = sizes
    tok, model = tokens.shape[1:]
    width = model // ranks
    narrow = width // BLOCKS
    wide = width + narrow
    hidden = w_gate.shape[3]
    chunks = micro * (experts // group)
    main_rows = group * ROWS
    extra_rows = max(ROWS, BLOCKS * group)
    rows = main_rows + extra_rows

    permute = np.zeros((BLOCKS, extra_rows, group, BLOCKS, BLOCKS), np.float32)
    for b in range(BLOCKS):
        for j in range(group):
            for k in range(BLOCKS):
                permute[b, j * BLOCKS + k, j, b, k] = 1.0
    permute = permute.reshape(BLOCKS * extra_rows, main_rows)
    pi = jnp.asarray(permute, BF16)
    pit = jnp.asarray(permute.T.copy(), BF16)

    vmem = pl.BlockSpec(memory_space=pltpu.VMEM)
    hbm = pl.BlockSpec(memory_space=pl.ANY)
    dma = pltpu.SemaphoreType.DMA
    out = pl.pallas_call(
        functools.partial(kernel, sizes),
        out_shape=jax.ShapeDtypeStruct((micro, tok, width), BF16),
        in_specs=[hbm] * 4 + [vmem] * 6,
        out_specs=vmem,
        scratch_shapes=[
            pltpu.VMEM((2, micro, experts * ROWS, tok), BF16),
            pltpu.VMEM((2, micro, experts * ROWS, BLOCKS * tok), BF16),
            pltpu.VMEM((micro, 2 * tok, experts * ROWS), BF16),
            pltpu.VMEM((micro, 2 * BLOCKS * tok, experts * ROWS), BF16),
            pltpu.VMEM((2, micro, experts, tok), F32),
            pltpu.VMEM((micro, tok, experts), F32),
            pltpu.VMEM((ranks, width, 2 * hidden), BF16),
            pltpu.VMEM((ranks, hidden, width), BF16),
            pltpu.VMEM((chunks, ranks, group, ROWS, wide), BF16),
            pltpu.VMEM((ranks, rows, width), BF16),
            pltpu.VMEM((rows, 2 * hidden), F32),
            pltpu.VMEM((chunks, ranks - 1, group, ROWS, wide), BF16),
            pltpu.VMEM((chunks, ranks, group, ROWS, wide), BF16),
            pltpu.VMEM((micro, experts, ROWS, wide), BF16),
            pltpu.VMEM((micro, experts, ROWS, wide), BF16),
            pltpu.VMEM((chunks, group, ROWS, wide), BF16),
            pltpu.VMEM((micro, experts, ROWS, wide), BF16),
            pltpu.VMEM((micro, tok, width), BF16),
            dma((3 * ranks,)),
            dma,
            dma((2, micro, experts)),
            dma((chunks, group)),
            dma((chunks, group, ranks - 1)),
            dma((chunks, ranks, group)),
            dma((chunks, ranks - 1)),
            dma((chunks, ranks)),
            dma((chunks, group)),
            dma((micro, experts)),
            dma((micro,)),
            dma((micro,)),
            dma,
            dma,
        ],
        compiler_params=pltpu.CompilerParams(
            collective_id=0, has_side_effects=True, vmem_limit_bytes=60_000_000
        ),
    )(
        tokens,
        w_gate[0, 0],
        w_up[0, 0],
        w_down[0, 0],
        gains.reshape(ranks, 1, width),
        jnp.swapaxes(route_ids[0], 1, 2),
        jnp.swapaxes(route_weights[0], 1, 2),
        picks[0],
        pi,
        pit,
    )
    return out[None]


def solution(mesh, group=2):
    experts = mesh.shape["expert"]
    sizes = (mesh.shape["pipe"], mesh.shape["tensor"], experts, 2, min(group, experts))
    return jax.shard_map(
        functools.partial(local, sizes),
        mesh=mesh,
        in_specs=(
            P(None, "expert", None),
            P("pipe", None),
            P("pipe", None, "expert", None),
            P("pipe", None, "expert", None),
            P("pipe", None, "expert", None),
            P("pipe", "expert", None, "tensor"),
            P("pipe", "expert", None, "tensor"),
            P("pipe", "expert", "tensor", None),
        ),
        out_specs=P("pipe", None, "expert", "tensor"),
        check_vma=False,
    )
```

```python
import functools

import jax
import jax.numpy as jnp
import numpy as np
from jax import lax
from jax.experimental import pallas as pl
from jax.experimental.pallas import tpu as pltpu
from jax.sharding import PartitionSpec as P

EPS = 1e-06
CAP = 5
ROWS = 16
BLOCKS = 4
F32 = jnp.float32
BF16 = jnp.bfloat16
MESH = pl.DeviceIdType.MESH


def dot(a, b):
    return jnp.dot(a, b, preferred_element_type=F32)


def kernel(
    sizes,
    tok_hbm,
    wg_hbm,
    wu_hbm,
    wd_hbm,
    gain_ref,
    ids_ref,
    wt_ref,
    row_ref,
    pi_ref,
    pit_ref,
    out_ref,
    pm_ref,
    pe_ref,
    cm_ref,
    ce_ref,
    post,
    pos_tok,
    w1,
    w2,
    x_buf,
    xs,
    acc,
    part_out,
    part_in,
    first_msg,
    next_msg,
    back_out,
    back_in,
    h_buf,
    w_sem,
    tok_sem,
    a1_send,
    a1_recv,
    a2_send,
    a2_recv,
    b1_send,
    b1_recv,
    b2_send,
    b2_recv,
    h_send,
    h_recv,
    post_send,
    post_recv,
):
    stages, ranks, experts, micro, group = sizes
    sets = experts // group
    chunks = micro * sets
    width = h_buf.shape[2]
    narrow = width // BLOCKS
    hidden = w2.shape[1]
    main_rows = group * ROWS
    extra_rows = xs.shape[1] - main_rows
    model = width * ranks
    tok = h_buf.shape[1]
    p = lax.axis_index("pipe")
    t = lax.axis_index("tensor")
    me = lax.axis_index("expert")
    my_set = lax.rem(me, sets)
    my_place = me // sets

    def peer(i):
        return lax.rem(t + i, ranks)

    def other(i):
        return lax.rem(me + i, experts)

    order = sorted(range(experts), key=lambda i: -min(i // 2, (experts - 1 - i) // 2 + 1 if i > 1 else 0))

    def other_chip(i):
        return lax.rem(me - lax.rem(me, 2) + i, experts)

    def remote(src, dst, send, recv, where):
        return pltpu.make_async_remote_copy(
            src_ref=src, dst_ref=dst, send_sem=send, recv_sem=recv, device_id=where, device_id_type=MESH
        )

    loads = []
    for f in range(ranks):
        rows = pl.ds(f * width, width)
        loads.append(pltpu.make_async_copy(wg_hbm.at[rows, :], w1.at[f, :, pl.ds(0, hidden)], w_sem.at[f]))
        loads.append(pltpu.make_async_copy(wu_hbm.at[rows, :], w1.at[f, :, pl.ds(hidden, hidden)], w_sem.at[ranks + f]))
        loads.append(pltpu.make_async_copy(wd_hbm.at[:, rows], w2.at[f], w_sem.at[2 * ranks + f]))
    slice_start = pl.multiple_of(t * width, 128)
    tok_load = pltpu.make_async_copy(tok_hbm.at[:, :, pl.ds(slice_start, width)], h_buf, tok_sem)

    @pl.when(p == 0)
    def _():
        tok_load.start()

    for load in loads:
        load.start()

    def count(shape, dim):
        return lax.broadcasted_iota(jnp.int32, shape, dim)

    def column(row):
        mine = count((tok, tok), 0) == count((tok, tok), 1)
        return jnp.sum(jnp.where(mine, row.astype(F32), 0.0), axis=1, keepdims=True)

    def slots(m):
        across, down = count((tok, tok), 1), count((tok, tok), 0)
        rank_row = jnp.sum(jnp.where(column(row_ref[m]) == across.astype(F32), down.astype(F32), 0.0), axis=0, keepdims=True)
        rank_col = jnp.sum(jnp.where(row_ref[m] == down, across.astype(F32), 0.0), axis=1, keepdims=True)
        part_row = jnp.floor(rank_row * (ranks / tok))
        part_col = jnp.floor(rank_col * (ranks / tok))
        same = jnp.where(part_row == part_col, 1.0, 0.0)
        before_t = (jnp.where(rank_col < rank_row, 1.0, 0.0) * same).astype(BF16)
        before = (jnp.where(rank_row < rank_col, 1.0, 0.0) * same).astype(BF16)
        e_down, e_across = count((experts, tok), 0), count((tok, experts), 1)
        ids = ids_ref[m]
        named_t = jnp.where((ids[0:1] == e_down) | (ids[1:2] == e_down), 1.0, 0.0)
        first, second = column(ids[0:1]), column(ids[1:2])
        e_across = e_across.astype(F32)
        named = jnp.where((first == e_across) | (second == e_across), 1.0, 0.0)
        slot_t = dot(named_t.astype(BF16), before_t)
        slot = dot(before, named.astype(BF16))
        post[0, m] = jnp.where((named_t > 0.0) & (slot_t < CAP), part_row * CAP + slot_t, -1.0)
        pos_tok[m] = jnp.where((named > 0.0) & (slot < CAP), part_col * CAP + slot, -1.0)

    def place(which, m):
        pos = post[which, m]
        four = jnp.concatenate([pos] * BLOCKS, axis=1)
        plain = count((ROWS, tok), 0).astype(F32)
        down, across = count((ROWS, BLOCKS * tok), 0), count((ROWS, BLOCKS * tok), 1)
        shift = tok.bit_length() - 1
        own = lax.shift_right_logical(across, shift) == lax.shift_right_logical(down, 2)
        slot = jnp.where(own, (ROWS + (down & 3)).astype(F32), -2.0)
        for e in range(experts):
            rows = pl.ds(e * ROWS, ROWS)
            pm_ref[which, m, rows, :] = jnp.where(pos[e : e + 1] == plain, 1.0, 0.0).astype(BF16)
            pe_ref[which, m, rows, :] = jnp.where(four[e : e + 1] == slot, 1.0, 0.0).astype(BF16)

    def gather(m):
        lanes = experts * ROWS
        e_across = count((tok, experts), 1).astype(F32)
        ids, wt = ids_ref[m], wt_ref[m]
        weight = jnp.where(column(ids[0:1]) == e_across, column(wt[0:1]), 0.0)
        weight = weight + jnp.where(column(ids[1:2]) == e_across, column(wt[1:2]), 0.0)
        high = weight.astype(BF16)
        low = (weight - high.astype(F32)).astype(BF16)
        block = lax.shift_right_logical(count((experts, lanes), 1), 4) == count((experts, lanes), 0)
        widen = jnp.where(block, 1.0, 0.0).astype(BF16)
        pos = dot(pos_tok[m].astype(BF16), widen)
        lane = count((tok, lanes), 1)
        inside = lane & (ROWS - 1)
        plain = inside.astype(F32)
        tail = (ROWS + (lane & 3)).astype(F32)
        for n, half in enumerate((high, low)):
            value = dot(half, widen)
            cm_ref[m, pl.ds(n * tok, tok), :] = jnp.where(pos == plain, value, 0.0).astype(BF16)
            for b in range(BLOCKS):
                mine = (pos == tail) & (lax.shift_right_logical(inside, 2) == b)
                ce_ref[m, pl.ds((n * BLOCKS + b) * tok, tok), :] = jnp.where(mine, value, 0.0).astype(BF16)

    for m in range(micro):
        slots(m)

    barrier = pltpu.get_barrier_semaphore()
    for i in range(1, ranks):
        pl.semaphore_signal(barrier, inc=1, device_id={"tensor": peer(i)}, device_id_type=MESH)
    for i in range(1, experts):
        pl.semaphore_signal(barrier, inc=1, device_id={"expert": other(i)}, device_id_type=MESH)

    @pl.when(p < stages - 1)
    def _():
        for e in range(experts):
            pl.semaphore_signal(barrier, inc=1, device_id={"pipe": p + 1, "expert": e}, device_id_type=MESH)

    @pl.when(p > 0)
    def _():
        for e in range(experts):
            pl.semaphore_signal(barrier, inc=1, device_id={"pipe": p - 1, "expert": e}, device_id_type=MESH)

    ahead = jnp.where(p < stages - 1, experts, 0)
    behind = jnp.where(p > 0, experts, 0)
    pl.semaphore_wait(barrier, ranks - 1 + experts - 1 + ahead + behind)

    def fill_messages(msg, which, m, stream):
        main = dot(pm_ref[which, m], stream).astype(BF16)
        stacked = jnp.concatenate([stream[:, b * narrow : (b + 1) * narrow] for b in range(BLOCKS)], axis=0)
        extra = dot(pe_ref[which, m], stacked).astype(BF16)
        for e in range(experts):
            msg[m, e, :, pl.ds(0, width)] = main[e * ROWS : (e + 1) * ROWS]
            msg[m, e, :, pl.ds(width, narrow)] = extra[e * ROWS : (e + 1) * ROWS]

    def first_copy(m, i):
        e = other(i)
        c = m * sets + my_set
        return remote(
            first_msg.at[m, e],
            x_buf.at[c, t, my_place],
            a1_send.at[0, m, e],
            a1_recv.at[c, my_place],
            {"expert": e},
        )

    def next_copy(m, e):
        c = m * sets + my_set
        return remote(
            next_msg.at[m, e],
            x_buf.at[c, t, my_place],
            a1_send.at[1, m, e],
            a1_recv.at[c, my_place],
            {"pipe": p + 1, "expert": e},
        )

    def post_copy():
        return remote(post.at[0], post.at[1], post_send, post_recv, {"pipe": p - 1})

    def stream_copy(m):
        return remote(out_ref.at[m], h_buf.at[m], h_send.at[m], h_recv.at[m], {"pipe": p + 1})

    def relay_copy(c, j, i):
        return remote(
            x_buf.at[c, t, j], x_buf.at[c, t, j], a2_send.at[c, j, i - 1], a2_recv.at[c, t, j], {"tensor": peer(i)}
        )

    def part_copy(c, i):
        return remote(
            part_out.at[c, i - 1], part_in.at[c, t], b1_send.at[c, i - 1], b1_recv.at[c, t], {"tensor": peer(i)}
        )

    def back_copy(c, j):
        m = c // sets
        g = j * sets + lax.rem(c, sets)
        return remote(back_out.at[c, j], back_in.at[m, me], b2_send.at[c, j], b2_recv.at[m, me], {"expert": g})

    def relay(c):
        near = lax.rem((me + experts - lax.rem(c, sets)) // 2, experts // 2) * 2 // sets
        for n in range(group):
            j = lax.rem(near + n, group)
            g = j * sets + lax.rem(c, sets)

            @pl.when((p > 0) | (g != me))
            def _():
                remote(
                    first_msg.at[0, 0], x_buf.at[c, t, j], a1_send.at[0, 0, 0], a1_recv.at[c, j], {"expert": other(1)}
                ).wait_recv()

            for i in (1, 3, 2):
                relay_copy(c, j, i).start()

    def experts_work(c):
        total = None
        squares = None
        for i in (0, 1, 3, 2):
            f = peer(i)
            if i > 0:
                for j in range(group):
                    remote(
                        x_buf.at[c, f, j], x_buf.at[c, f, j], a2_send.at[c, j, i - 1], a2_recv.at[c, f, j], {"tensor": f}
                    ).wait_recv()
            gain = gain_ref[f]
            main = x_buf[c, f, :, :, pl.ds(0, width)].reshape(main_rows, width).astype(F32)
            xs[f, pl.ds(0, main_rows), :] = (main * gain).astype(BF16)
            packed = x_buf[c, f, :, :, pl.ds(width, narrow)].reshape(main_rows, narrow)
            extra = dot(pi_ref[...], packed)
            extra_sq = jnp.zeros((extra_rows, 1), F32)
            for b in range(BLOCKS):
                block = extra[b * extra_rows : (b + 1) * extra_rows]
                cols = slice(b * narrow, (b + 1) * narrow)
                extra_sq = extra_sq + jnp.sum(block * block, axis=1, keepdims=True)
                xs[f, pl.ds(main_rows, extra_rows), pl.ds(b * narrow, narrow)] = (block * gain[:, cols]).astype(BF16)
            sq = jnp.concatenate([jnp.sum(main * main, axis=1, keepdims=True), extra_sq], axis=0)
            squares = sq if squares is None else squares + sq
            if i == 0:
                acc[...] = dot(xs[f], w1[f])
            else:
                acc[...] += dot(xs[f], w1[f])
        inv = lax.rsqrt(squares * (1.0 / model) + EPS)
        gate = acc[:, pl.ds(0, hidden)] * inv
        up = acc[:, pl.ds(hidden, hidden)] * inv
        act = (gate / (1.0 + jnp.exp(-gate)) * up).astype(BF16)
        for i in (1, 3, 2, 0):
            part = dot(act, w2[peer(i)]).astype(BF16)
            extra = part[main_rows:]
            stacked = jnp.concatenate([extra[:, b * narrow : (b + 1) * narrow] for b in range(BLOCKS)], axis=0)
            packed = dot(pit_ref[...], stacked).astype(BF16)
            wide = jnp.concatenate([part[:main_rows], packed], axis=1).reshape(group, ROWS, width + narrow)
            if i == 0:
                part_in[c, t] = wide
            else:
                part_out[c, i - 1] = wide
                part_copy(c, i).start()

    def give_back(c):
        m = c // sets
        for i in range(1, ranks):
            f = peer(i)
            remote(part_out.at[c, i - 1], part_in.at[c, f], b1_send.at[c, i - 1], b1_recv.at[c, f], {"tensor": f}).wait_recv()
        total = part_in[c, 0].astype(F32)
        for q in range(1, ranks):
            total = total + part_in[c, q].astype(F32)
        back_out[c] = total.astype(BF16)
        for j in range(group):
            g = j * sets + lax.rem(c, sets)

            @pl.when(g != me)
            def _():
                back_copy(c, j).start()

            @pl.when(g == me)
            def _():
                back_in[m, me] = back_out[c, j]

    def combine(c):
        m = c // sets

        @pl.when(lax.rem(c, sets) == my_set)
        def _():
            for i in range(1, experts):
                e = other(i)
                remote(back_out.at[c, 0], back_in.at[m, e], b2_send.at[c, 0], b2_recv.at[m, e], {"expert": e}).wait_recv()

            @pl.when(p > 0)
            def _():
                remote(out_ref.at[m], h_buf.at[m], h_send.at[m], h_recv.at[m], {"expert": other(1)}).wait_recv()

            main = back_in[m, :, :, pl.ds(0, width)].reshape(experts * ROWS, width)
            packed = back_in[m, :, :, pl.ds(width, narrow)].reshape(experts * ROWS, narrow)
            wide = dot(cm_ref[m], main)
            update = wide[:tok] + wide[tok:]
            thin = dot(ce_ref[m], packed)
            thin = thin[: BLOCKS * tok] + thin[BLOCKS * tok :]
            spread = jnp.concatenate([thin[b * tok : (b + 1) * tok] for b in range(BLOCKS)], axis=1)
            fresh = (h_buf[m].astype(F32) + update + spread).astype(BF16)
            out_ref[m] = fresh

            @pl.when(p < stages - 1)
            def _():
                fill_messages(next_msg, 1, m, fresh)
                for i in order:
                    next_copy(m, other_chip(i)).start()
                stream_copy(m).start()

    @pl.when(p > 0)
    def _():
        post_copy().start()

    def start(m):
        fill_messages(first_msg, 0, m, h_buf[m])
        for i in sorted(range(1, experts), key=lambda i: abs(2 * i - experts)):
            first_copy(m, i).start()
        x_buf[m * sets + my_set, t, my_place] = first_msg[m, me]

    @pl.when(p == 0)
    def _():
        tok_load.wait()
        for m in range(micro):
            place(0, m)

        @pl.when(my_set == 0)
        def _():
            start(0)

    for m in range(micro):
        gather(m)

    @pl.when(p < stages - 1)
    def _():
        remote(post.at[0], post.at[1], post_send, post_recv, {"expert": other(1)}).wait_recv()
        for m in range(micro):
            place(1, m)

    @pl.when(p == 0)
    def _():
        @pl.when(my_set > 0)
        def _():
            start(0)

        for m in range(1, micro):
            start(m)

    for load in loads:
        load.wait()

    def step(s, carry):
        @pl.when(s < chunks)
        def _():
            relay(s)

        @pl.when(s > 0)
        def _():
            give_back(s - 1)

        @pl.when(s < chunks)
        def _():
            experts_work(s)

        @pl.when(s > 0)
        def _():
            combine(s - 1)

        return carry

    lax.fori_loop(0, chunks + 1, step, 0)

    @pl.when(p > 0)
    def _():
        post_copy().wait_send()

    @pl.when(p == 0)
    def _():
        for m in range(micro):
            for i in range(1, experts):
                first_copy(m, i).wait_send()

    @pl.when(p < stages - 1)
    def _():
        for m in range(micro):
            for e in range(experts):
                next_copy(m, e).wait_send()
            stream_copy(m).wait_send()

    def drain(c, carry):
        for j in range(group):
            for i in range(1, ranks):
                relay_copy(c, j, i).wait_send()
            g = j * sets + lax.rem(c, sets)

            @pl.when(g != me)
            def _():
                back_copy(c, j).wait_send()

        for i in range(1, ranks):
            part_copy(c, i).wait_send()
        return carry

    lax.fori_loop(0, chunks, drain, 0)


def local(sizes, tokens, gains, route_ids, route_weights, picks, w_gate, w_up, w_down):
    stages, ranks, experts, micro, group = sizes
    tok, model = tokens.shape[1:]
    width = model // ranks
    narrow = width // BLOCKS
    wide = width + narrow
    hidden = w_gate.shape[3]
    chunks = micro * (experts // group)
    main_rows = group * ROWS
    extra_rows = max(ROWS, BLOCKS * group)
    rows = main_rows + extra_rows

    permute = np.zeros((BLOCKS, extra_rows, group, BLOCKS, BLOCKS), np.float32)
    for b in range(BLOCKS):
        for j in range(group):
            for k in range(BLOCKS):
                permute[b, j * BLOCKS + k, j, b, k] = 1.0
    permute = permute.reshape(BLOCKS * extra_rows, main_rows)
    pi = jnp.asarray(permute, BF16)
    pit = jnp.asarray(permute.T.copy(), BF16)

    vmem = pl.BlockSpec(memory_space=pltpu.VMEM)
    hbm = pl.BlockSpec(memory_space=pl.ANY)
    dma = pltpu.SemaphoreType.DMA
    out = pl.pallas_call(
        functools.partial(kernel, sizes),
        out_shape=jax.ShapeDtypeStruct((micro, tok, width), BF16),
        in_specs=[hbm] * 4 + [vmem] * 6,
        out_specs=vmem,
        scratch_shapes=[
            pltpu.VMEM((2, micro, experts * ROWS, tok), BF16),
            pltpu.VMEM((2, micro, experts * ROWS, BLOCKS * tok), BF16),
            pltpu.VMEM((micro, 2 * tok, experts * ROWS), BF16),
            pltpu.VMEM((micro, 2 * BLOCKS * tok, experts * ROWS), BF16),
            pltpu.VMEM((2, micro, experts, tok), F32),
            pltpu.VMEM((micro, tok, experts), F32),
            pltpu.VMEM((ranks, width, 2 * hidden), BF16),
            pltpu.VMEM((ranks, hidden, width), BF16),
            pltpu.VMEM((chunks, ranks, group, ROWS, wide), BF16),
            pltpu.VMEM((ranks, rows, width), BF16),
            pltpu.VMEM((rows, 2 * hidden), F32),
            pltpu.VMEM((chunks, ranks - 1, group, ROWS, wide), BF16),
            pltpu.VMEM((chunks, ranks, group, ROWS, wide), BF16),
            pltpu.VMEM((micro, experts, ROWS, wide), BF16),
            pltpu.VMEM((micro, experts, ROWS, wide), BF16),
            pltpu.VMEM((chunks, group, ROWS, wide), BF16),
            pltpu.VMEM((micro, experts, ROWS, wide), BF16),
            pltpu.VMEM((micro, tok, width), BF16),
            dma((3 * ranks,)),
            dma,
            dma((2, micro, experts)),
            dma((chunks, group)),
            dma((chunks, group, ranks - 1)),
            dma((chunks, ranks, group)),
            dma((chunks, ranks - 1)),
            dma((chunks, ranks)),
            dma((chunks, group)),
            dma((micro, experts)),
            dma((micro,)),
            dma((micro,)),
            dma,
            dma,
        ],
        compiler_params=pltpu.CompilerParams(
            collective_id=0, has_side_effects=True, vmem_limit_bytes=60_000_000
        ),
    )(
        tokens,
        w_gate[0, 0],
        w_up[0, 0],
        w_down[0, 0],
        gains.reshape(ranks, 1, width),
        jnp.swapaxes(route_ids[0], 1, 2),
        jnp.swapaxes(route_weights[0], 1, 2),
        picks[0],
        pi,
        pit,
    )
    return out[None]


def solution(mesh, group=2):
    experts = mesh.shape["expert"]
    sizes = (mesh.shape["pipe"], mesh.shape["tensor"], experts, 2, min(group, experts))
    return jax.shard_map(
        functools.partial(local, sizes),
        mesh=mesh,
        in_specs=(
            P(None, "expert", None),
            P("pipe", None),
            P("pipe", None, "expert", None),
            P("pipe", None, "expert", None),
            P("pipe", None, "expert", None),
            P("pipe", "expert", None, "tensor"),
            P("pipe", "expert", None, "tensor"),
            P("pipe", "expert", "tensor", None),
        ),
        out_specs=P("pipe", None, "expert", "tensor"),
        check_vma=False,
    )
```
